128 devices in a mesh: section: 4 (over y_hi, core), fsdp: 32 (over z, x, y_lo).
Axes of the slice: x: 4, y: 4 (y_hi: 2, y_lo: 2; y = y_hi * 2 + y_lo), z: 4, core: 2. Of those that a mesh axis runs over, the one named last changes fastest.
Arguments:
- hidden_in: bfloat16 [4096, 4096], P('fsdp'), may hold values from -6 to 6
- out_grad: bfloat16 [4096, 4096], P('fsdp'), may hold values from -6 to 6
- fast_in: float32 [4, 4096, 1024], P('section', 'fsdp'), may hold values from -6 to 6
- fast_out: float32 [4, 1024, 4096], P('section', None, 'fsdp'), may hold values from -6 to 6
- slow_in: float32 [4, 4096, 1024], P('section', 'fsdp'), may hold values from -6 to 6
- slow_out: float32 [4, 1024, 4096], P('section', None, 'fsdp'), may hold values from -6 to 6
Outputs:
- section_out: bfloat16 [4, 4096, 4096], P('section', 'fsdp')
- input_grad: bfloat16 [4, 4096, 4096], P('section', 'fsdp')
- synced_in: float32 [4, 4096, 1024], P('section', 'fsdp')
- synced_out: float32 [4, 1024, 4096], P('section', None, 'fsdp')
The draws below stay inside these ranges and needn't reach their ends.
All inputs are finite; a program needn't handle non-finite values.
Results may differ from the reference program's by a relative error of at most 0.014.
Values may be sent and summed in bfloat16 or wider, within the bound.
A program may use at most 896 MiB of HBM per device.

```python
import math
import jax
import jax.numpy as jnp
from jax import lax

D = 4096
LAT = 1024
TOK_DEV = 128
TOKENS = 4096
LAYERS = 4
N_SECTION = 4
N_FSDP = 32


def raised(entries, stream_key, source, target, parts, factor):
    owner, partner = [(jnp.arange(entries.shape[axis_at]) // (entries.shape[axis_at] // parts)).reshape([-1 if axis == axis_at else 1 for axis in range(entries.ndim)]) for axis_at in (source, target)]
    chosen = jax.random.permutation(stream_key, parts)[partner]
    strong = (owner == chosen) | (owner == (partner + parts // 2) % parts)
    return jnp.where(strong, factor * entries, entries)


def level_of(stream_key, shape, split, low, largest):
    def one(axis_at, parts):
        steps = jax.random.uniform(jax.random.fold_in(jax.random.fold_in(stream_key, 6), axis_at), (parts,), jnp.float32, low / len(split), largest / len(split))
        return jnp.repeat(jnp.exp(steps), shape[axis_at] // parts).reshape((-1,) + (1,) * (len(shape) - axis_at - 1))

    level = one(*split[0])
    for cut in split[1:]:
        level = level * one(*cut)
    return level


def centred(stream_key, dims, deviation, reach, shards=(), kind=jnp.bfloat16):
    entries = jax.random.normal(stream_key, dims, jnp.float32) * deviation
    if len(shards) > 0:
        entries = level_of(stream_key, dims, shards, -0.22, 0.18) * entries
    return jnp.clip(entries, min=-reach, max=reach).astype(kind)


def gaussian_with(own_key, shape, width, reach, cuts, heavy, kind=jnp.bfloat16):
    array = width * jax.random.normal(own_key, shape, jnp.float32)
    if cuts:
        array = array * level_of(own_key, shape, cuts, -0.22, 0.18)
    return jnp.clip(raised(array, jax.random.fold_in(own_key, 3), *heavy), -reach, reach).astype(kind)


def setup_inputs(seed: int = 0) -> dict:
    seeds = jax.random.split(jax.random.key(seed), 7)
    hidden_in = gaussian_with(seeds[0], (TOKENS, D), 1.0, 6.0, ((0, 32),), (0, 1, 32, 2.75))
    out_grad = centred(seeds[1], (TOKENS, D), 1.0, 6.0, ((0, 32),))
    fast_in = centred(seeds[2], (LAYERS, D, LAT), 1.0, 6.0, ((0, 4), (1, 32)), jnp.float32)
    fast_out = centred(seeds[3], (LAYERS, LAT, D), 1.0, 6.0, ((0, 4), (2, 32)), jnp.float32)
    slow_in = centred(seeds[4], (LAYERS, D, LAT), 1.0, 6.0, ((0, 4), (1, 32)), jnp.float32)
    slow_out = centred(seeds[5], (LAYERS, LAT, D), 1.0, 6.0, ((0, 4), (2, 32)), jnp.float32)
    return {"hidden_in": hidden_in, "out_grad": out_grad, "fast_in": fast_in, "fast_out": fast_out, "slow_in": slow_in, "slow_out": slow_out}


epsilon = 1e-05
fast_rate = 0.5
preview_mix = 0.5

def contract_last(left_rows, right_rows):
    return lax.dot_general(left_rows, right_rows, (((1,), (1,)), ((), ())), preferred_element_type=jnp.float32)

def contract_first(left_rows, right_rows):
    return lax.dot_general(left_rows, right_rows, (((0,), (0,)), ((), ())), preferred_element_type=jnp.float32)

def prepare(hidden, weight_in):
    widened = hidden.astype(jnp.float32)
    inverse_rms = lax.rsqrt(lax.optimization_barrier(jnp.mean(widened * widened, axis=-1, keepdims=True)) + epsilon)
    normed = (widened * inverse_rms).astype(jnp.bfloat16)
    pre_act = jnp.dot(normed, weight_in, preferred_element_type=jnp.float32)
    activated = jax.nn.silu(pre_act).astype(jnp.bfloat16)
    return (widened, inverse_rms, normed, pre_act, activated)

def advance(hidden, weight_in, weight_out):
    widened, inverse_rms, normed, pre_act, activated = prepare(hidden, weight_in)
    return (widened + jnp.dot(activated, weight_out, preferred_element_type=jnp.float32)).astype(jnp.bfloat16)

def retreat(hidden, cot_in, weight_in, weight_out):
    widened, inverse_rms, normed, pre_act, activated = prepare(hidden, weight_in)
    act_grad = contract_last(cot_in, weight_out)
    sigmoid_vals = jax.nn.sigmoid(pre_act)
    pre_grad = (act_grad * sigmoid_vals * (1.0 + pre_act * (1.0 - sigmoid_vals))).astype(jnp.bfloat16)
    norm_grad = contract_last(pre_grad, weight_in)
    unit_rows = widened * inverse_rms
    rms_grad = inverse_rms * (norm_grad - unit_rows * lax.optimization_barrier(jnp.mean(norm_grad * unit_rows, axis=-1, keepdims=True)))
    earlier = (cot_in.astype(jnp.float32) + rms_grad).astype(jnp.bfloat16)
    return (earlier, normed, pre_grad, activated)

def shard_sum(left_rows, right_rows, factor):
    pieces_left = left_rows.reshape(N_FSDP, TOK_DEV, left_rows.shape[1])
    pieces_right = right_rows.reshape(N_FSDP, TOK_DEV, right_rows.shape[1])

    def accumulate(running, operands):
        partial_value = contract_first(operands[0], operands[1]) * factor
        rounded = lax.optimization_barrier(partial_value.astype(jnp.bfloat16))
        return (running + rounded.astype(jnp.float32), None)
    start = jnp.zeros((left_rows.shape[1], right_rows.shape[1]), jnp.float32)
    running, ignored = lax.scan(accumulate, start, (pieces_left, pieces_right))
    return running

def reference(hidden_in, out_grad, fast_in, fast_out, slow_in, slow_out):
    in_scale = 1.0 / math.sqrt(D)
    out_scale = 1.0 / math.sqrt(LAT)
    weights_in = [(fast_in[layer_index] * in_scale).astype(jnp.bfloat16) for layer_index in range(N_SECTION)]
    weights_out = [(fast_out[layer_index] * out_scale).astype(jnp.bfloat16) for layer_index in range(N_SECTION)]
    inputs = []
    outputs = []
    current = hidden_in
    for layer_index in range(N_SECTION):
        inputs.append(current)
        current = advance(current, weights_in[layer_index], weights_out[layer_index])
        outputs.append(current)
    cot_in = out_grad
    cotangents = [None] * N_SECTION
    synced_first = [None] * N_SECTION
    synced_second = [None] * N_SECTION
    for layer_index in reversed(range(N_SECTION)):
        earlier, normed, pre_grad, activated = retreat(inputs[layer_index], cot_in, weights_in[layer_index], weights_out[layer_index])
        grad_in = shard_sum(normed, pre_grad, in_scale)
        grad_out = shard_sum(activated, cot_in, out_scale)
        fresh_in = fast_in[layer_index] - fast_rate * grad_in
        fresh_out = fast_out[layer_index] - fast_rate * grad_out
        synced_first[layer_index] = slow_in[layer_index] + preview_mix * (fresh_in - slow_in[layer_index])
        synced_second[layer_index] = slow_out[layer_index] + preview_mix * (fresh_out - slow_out[layer_index])
        cotangents[layer_index] = earlier
        cot_in = earlier
    return (jnp.stack(outputs), jnp.stack(cotangents), jnp.stack(synced_first), jnp.stack(synced_second))
```

```python
import functools
import math

import jax
import jax.numpy as jnp
from jax import lax
from jax.experimental import pallas as pl
from jax.experimental.pallas import tpu as pltpu
from jax.sharding import PartitionSpec as P

EPS = 1e-05
RATE = 0.5
MIX = 0.5
MESH = pl.DeviceIdType.MESH
BF = jnp.bfloat16
F32 = jnp.float32
EXT = 128


def split_lanes(column):
    high = column.astype(BF)
    low = (column - high.astype(F32)).astype(BF)
    lane = lax.broadcasted_iota(jnp.int32, (column.shape[0], EXT), 1)
    return jnp.where(lane < EXT // 2, high.astype(F32), low.astype(F32)).astype(BF)


def join_lanes(lanes):
    return jnp.sum(lanes.astype(F32), axis=-1, keepdims=True) * (2.0 / EXT)


def relay(
    hid_hbm, cot_hbm, fin_hbm, fout_hbm,
    so_hbm, ig_hbm, gw_ref,
    fin, fout, hid, cot, stage0, W, G, Gx, h, g, stg, land, act, pgb, pre, rinv,
    z1, z2, za, zb, gw,
    in_sem, s_send, s_recv,
):
    D, LAT = 4096, 1024
    in_scale, out_scale = 1.0 / math.sqrt(D), 1.0 / math.sqrt(LAT)
    s = lax.axis_index("section")
    f = lax.axis_index("fsdp")
    core, yh = s % 2, s // 2
    z, x, yl = f // 8, (f // 2) % 4, f % 2
    y = yh * 2 + yl
    other = 1 - core

    def dev(yy, zz, xx, cc):
        return ((yy // 2) * 2 + cc, zz * 8 + xx * 2 + yy % 2)

    counters = {"s": 0, "r": 0}
    sends = []

    def sem(kind, n=1):
        at = counters[kind]
        counters[kind] += n
        return at

    def push(src, dst, recv_index, to):
        copy = pltpu.make_async_remote_copy(
            src_ref=src, dst_ref=dst, send_sem=s_send.at[sem("s")], recv_sem=s_recv.at[recv_index],
            device_id=to, device_id_type=MESH,
        )
        copy.start()
        sends.append(copy)

    def got(dst, recv_index):
        pltpu.make_async_remote_copy(
            src_ref=dst, dst_ref=dst, send_sem=s_send.at[0], recv_sem=s_recv.at[recv_index],
            device_id=(s, f), device_id_type=MESH,
        ).wait_recv()

    rows = pl.ds(pl.multiple_of(s * 32, 32), 32)
    loads = [
        pltpu.make_async_copy(fin_hbm.at[0], fin, in_sem.at[0]),
        pltpu.make_async_copy(fout_hbm.at[0], fout, in_sem.at[1]),
        pltpu.make_async_copy(hid_hbm.at[rows], hid, in_sem.at[2]),
        pltpu.make_async_copy(cot_hbm.at[rows], cot, in_sem.at[3]),
    ]
    for c in loads:
        c.start()

    yp, ym, zp, zm = (y + 1) % 4, (y + 3) % 4, (z + 1) % 4, (z + 3) % 4
    to_yp, to_ym = dev(yp, z, x, core), dev(ym, z, x, core)
    to_zp, to_zm = dev(y, zp, x, core), dev(y, zm, x, core)
    partner = dev(y, z, x, other)
    barrier = pltpu.get_barrier_semaphore()
    greeted = [to_yp, to_ym, to_zp, to_zm]
    for ds in range(4):
        for dx in range(4):
            if ds or dx:
                greeted.append(((s + ds) % 4, z * 8 + ((x + dx) % 4) * 2 + yl))
    for to in greeted:
        pl.semaphore_signal(barrier, inc=1, device_id=to, device_id_type=MESH)
    pl.semaphore_wait(barrier, len(greeted))

    def xdev(d):
        return (s, z * 8 + ((x + d) % 4) * 2 + yl)

    loads[0].wait()
    W[yh, core, 0, z, yl] = (fin[...] * in_scale).astype(BF)
    loads[1].wait()
    W[yh, core, 1, z, yl] = (fout[...] * out_scale).T.astype(BF)
    own_recv = sem("r", 2)
    for k in range(2):
        ref = W.at[yh, core, k, z, yl]
        push(ref, ref, own_recv + k, partner)

    def spread(source, target, load):
        load.wait()
        base = sem("r", 4)
        slot = 0 if target is h else 1
        for xx in range(4):
            for zz in range(4):
                stage0[slot, xx, :, zz * 256:(zz + 1) * 256] = source[:, zz * 1024 + xx * 256: zz * 1024 + (xx + 1) * 256]
        level = 0 if target is h else 4
        target[level, x] = stage0[slot, x]
        for d in (1, 3, 2):
            push(stage0.at[slot, (x + d) % 4], target.at[level, x], base + d, xdev(d))
        return base

    def ag_ring(item, half, q, to_plus, to_minus):
        base = sem("r", 8)
        qp, qm, qo = (q + 1) % 4, (q + 3) % 4, (q + 2) % 4
        push(item(q), item(q), base + 0, to_plus)
        push(item(q), item(q), base + 1, to_minus)
        yield
        got(item(qm), base + 0)
        push(half(qm, 0), half(qm, 0), base + 2, to_plus)
        push(item(qm), item(qm), base + 4, partner)
        yield
        got(item(qp), base + 1)
        push(half(qp, 1), half(qp, 1), base + 3, to_minus)
        push(item(qp), item(qp), base + 5, partner)
        yield
        got(half(qo, 0), base + 2)
        push(half(qo, 0), half(qo, 0), base + 6, partner)
        yield
        got(half(qo, 1), base + 3)
        push(half(qo, 1), half(qo, 1), base + 7, partner)
        pending.append(lambda: twin(item, half, q, base))

    pending = []

    def twin(item, half, q, base):
        qp, qm, qo = (q + 1) % 4, (q + 3) % 4, (q + 2) % 4
        got(item(qm, other), base + 4)
        got(item(qp, other), base + 5)
        got(half(qo, 0, other), base + 6)
        got(half(qo, 1, other), base + 7)

    def ag_round(r):
        def item_a1(c, k=core):
            return W.at[c // 2, r, k, z, c % 2, 0:64]

        def half_a1(c, n, k=core):
            return W.at[c // 2, r, k, z, c % 2, 32 * n:32 * n + 32]

        def item_b1(c, k=core):
            return W.at[yh, r, k, c, yl, 64:128]

        def half_b1(c, n, k=core):
            return W.at[yh, r, k, c, yl, 64 + 32 * n:96 + 32 * n]

        def item_a2(c, k=core):
            return W.at[:, r, k, c, :, 0:64]

        def half_a2(c, n, k=core):
            return W.at[n, r, k, c, :, 0:64]

        def item_b2(c, k=core):
            return W.at[c // 2, r, k, :, c % 2, 64:128]

        def half_b2(c, n, k=core):
            return W.at[c // 2, r, k, 2 * n:2 * n + 2, c % 2, 64:128]

        first = [ag_ring(item_a1, half_a1, y, to_yp, to_ym), ag_ring(item_b1, half_b1, z, to_zp, to_zm)]
        yield from zipped(first)
        second = [ag_ring(item_a2, half_a2, z, to_zp, to_zm), ag_ring(item_b2, half_b2, y, to_yp, to_ym)]
        yield from zipped(second)

    def zipped(tasks):
        tasks = list(tasks)
        while tasks:
            for t in list(tasks):
                try:
                    next(t)
                except StopIteration:
                    tasks.remove(t)
            yield

    def drain(task):
        for _ in task:
            pass

    def wtile(l, k, c0, n):
        return W[l // 2, l % 2, k, :, :, :, c0:c0 + n].reshape(1024, n)

    def dot_nn(a, b):
        return lax.dot_general(a, b, (((1,), (0,)), ((), ())), preferred_element_type=F32)

    def dot_nt(a, b):
        return lax.dot_general(a, b, (((1,), (1,)), ((), ())), preferred_element_type=F32)

    def dot_tn(a, b):
        return lax.dot_general(a, b, (((0,), (0,)), ((), ())), preferred_element_type=F32)

    NT = 256

    def project(source, level, l, k, step):
        left = source[level].reshape(128, 1024)

        def body(i, carry):
            c = pl.multiple_of(i * NT, NT)
            right = W[l // 2, l % 2, k, :, :, :, pl.ds(c, NT)].reshape(1024, NT)
            stg[step, :, :, pl.ds(c, NT)] = dot_nn(left, right).astype(BF).reshape(4, 32, NT)
            return carry
        lax.fori_loop(0, LAT // NT, body, 0)

    def scatter(step):
        base = sem("r", 4)
        land[step, x] = stg[step, x]
        for d in (2, 1, 3):
            push(stg.at[step, (x + d) % 4], land.at[step, x], base + d, xdev(d))
        return base

    def summed(step, base):
        for d in (1, 3, 2):
            got(land.at[step, (x + 4 - d) % 4], base + d)

    def broadcast(buf, l):
        base = sem("r", 4)
        for d in (2, 1, 3):
            push(buf.at[l, x], buf.at[l, x], base + d, xdev(d))
        return base

    def collect(buf, l, base):
        for d in (1, 3, 2):
            got(buf.at[l, (x + 4 - d) % 4], base + d)

    def emit(source, level, l, out_ref):
        base = sem("r", 16)
        mine = s * 4 + x
        for d in range(4):
            src = source.at[level, (x + d) % 4]
            dst = out_ref.at[x, rows]
            to = (l, z * 8 + ((x + d) % 4) * 2 + yl)
            copy = pltpu.make_async_remote_copy(
                src_ref=src, dst_ref=dst, send_sem=s_send.at[sem("s")], recv_sem=s_recv.at[base + mine],
                device_id=to, device_id_type=MESH,
            )
            if d:
                copy.start()
                sends.append(copy)
            else:
                local = pltpu.make_async_copy(src, dst, in_sem.at[4 + sem("l")])

                @pl.when(s != l)
                def _():
                    copy.start()

                @pl.when(s == l)
                def _():
                    local.start()
                locals_.append((l, copy, local))
        emitted.append((l, base, out_ref))

    counters["l"] = 0
    locals_, emitted = [], []

    def finish_emit():
        for l, copy, local in locals_:
            @pl.when(s != l)
            def _():
                copy.wait_send()

            @pl.when(s == l)
            def _():
                local.wait()
        for l, base, out_ref in emitted:
            @pl.when(s == l)
            def _():
                for ds in range(4):
                    for dx in range(4):
                        if ds or dx:
                            ss, xx = (s + ds) % 4, (x + dx) % 4
                            got(out_ref.at[xx, pl.ds(pl.multiple_of(ss * 32, 32), 32)], base + ss * 4 + xx)

    def forward(l):
        project(h, l, l, 0, l)
        wide = h[l].reshape(128, 1024).astype(F32)
        ss = jnp.sum(wide * wide, axis=-1, keepdims=True)
        stg[l, :, :, LAT:] = split_lanes(ss).reshape(4, 32, EXT)
        base = scatter(l)
        yield
        summed(l, base)
        total = land[l, 0].astype(F32)
        for xx in range(1, 4):
            total = total + land[l, xx].astype(F32)
        r = lax.rsqrt(join_lanes(total[:, LAT:]) * (1.0 / D) + EPS)
        v = total[:, :LAT] * r
        pre[l] = v
        rinv[l] = jnp.broadcast_to(r, (32, EXT))
        act[l, x] = (v / (1.0 + jnp.exp(-v))).astype(BF)
        base = broadcast(act, l)
        yield
        collect(act, l, base)
        left = act[l].reshape(128, 1024)

        def body(i, carry):
            c = pl.multiple_of(i * NT, NT)
            right = W[l // 2, l % 2, 1, i].reshape(NT, 1024)
            old = h[l, :, :, pl.ds(c, NT)].reshape(128, NT).astype(F32)
            h[l + 1, :, :, pl.ds(c, NT)] = (old + dot_nt(left, right)).astype(BF).reshape(4, 32, NT)
            return carry
        lax.fori_loop(0, 4, body, 0)
        emit(h, l + 1, l, so_hbm)

    def wgrad(l, kind, left_ref, left_level, right_ref, scale):
        right = right_ref[l, :, :, :LAT].reshape(128, LAT)

        def body(i, carry):
            c = pl.multiple_of(i * 128, 128)
            left = left_ref[left_level, :, :, pl.ds(c, 128)].reshape(128, 128)
            value = (dot_tn(left, right) * scale).astype(BF)
            G[l // 2, l % 2, kind, i // 2, i % 2] = value
            return carry
        lax.fori_loop(0, 8, body, 0)

    def backward(l):
        step = 7 - l
        project(g, l + 1, l, 1, step)
        base = scatter(step)
        yield
        wgrad(l, 1, g, l + 1, act, out_scale)
        summed(step, base)
        total = land[step, 0, :, :LAT].astype(F32)
        for xx in range(1, 4):
            total = total + land[step, xx, :, :LAT].astype(F32)
        v = pre[l]
        r = rinv[l][:, :1]
        sg = 1.0 / (1.0 + jnp.exp(-v))
        scaled = (r * (total * sg * (1.0 + v * (1.0 - sg)))).astype(BF)
        kappa = r * jnp.sum(scaled.astype(F32) * v, axis=-1, keepdims=True) * (1.0 / D)
        pgb[l, x, :, :LAT] = scaled
        pgb[l, x, :, LAT:] = split_lanes(kappa)
        base = broadcast(pgb, l)
        yield
        collect(pgb, l, base)
        left = pgb[l, :, :, :LAT].reshape(128, LAT)
        kap = join_lanes(pgb[l, :, :, LAT:].reshape(128, EXT))

        def body(i, carry):
            c = pl.multiple_of(i * NT, NT)
            right = W[l // 2, l % 2, 0, i].reshape(NT, 1024)
            old = g[l + 1, :, :, pl.ds(c, NT)].reshape(128, NT).astype(F32)
            base_h = h[l, :, :, pl.ds(c, NT)].reshape(128, NT).astype(F32)
            g[l, :, :, pl.ds(c, NT)] = (old + dot_nt(left, right) - base_h * kap).astype(BF).reshape(4, 32, NT)
            return carry
        lax.fori_loop(0, 4, body, 0)
        emit(g, l, l, ig_hbm)
        wgrad(l, 0, h, l, pgb, in_scale)
        gx_base[l] = sem("r")
        push(G.at[l // 2, l % 2, other], Gx.at[l // 2, l % 2], gx_base[l], partner)

    gx_base = {}

    def merge(l):
        got(Gx.at[l // 2, l % 2], gx_base[l])

        def body(i, carry):
            G[l // 2, l % 2, core, i // 2, i % 2] = G[l // 2, l % 2, core, i // 2, i % 2] + Gx[l // 2, l % 2, i // 2, i % 2]
            return carry
        lax.fori_loop(0, 8, body, 0)

    def rs_ring(half, lands, q, to_plus, to_minus, parts, result):
        p1, m1, p2, m2 = lands
        base = sem("r", 6)
        qp, qm, qo = (q + 1) % 4, (q + 3) % 4, (q + 2) % 4
        push(half(qo, 0), p1, base + 0, to_plus)
        push(half(qo, 1), m1, base + 1, to_minus)
        push(half(qp, 1), p2(1), base + 2, to_plus)
        push(half(qm, 0), m2(0), base + 3, to_minus)
        yield
        got(p1, base + 0)
        parts(half(qp, 0), half(qp, 0), [p1])
        push(half(qp, 0), p2(0), base + 4, to_plus)
        yield
        got(m1, base + 1)
        parts(half(qm, 1), half(qm, 1), [m1])
        push(half(qm, 1), m2(1), base + 5, to_minus)
        yield
        got(m2(0), base + 3)
        got(p2(1), base + 2)
        got(p2(0), base + 4)
        parts(half(q, 0), result(0), [p2(0), m2(0)])
        yield
        got(m2(1), base + 5)
        parts(half(q, 1), result(1), [p2(1), m2(1)])

    def add_flat(shape):
        count = math.prod(shape)

        def run(own, out, terms):
            def body(i, carry):
                index, rest = [], i
                for n in reversed(shape):
                    index.insert(0, rest % n)
                    rest = rest // n
                index = tuple(index)
                value = own[index] if index else own[...]
                value = value.astype(F32)
                for t in terms:
                    value = value + (t[index] if index else t[...]).astype(F32)
                if index:
                    out[index] = value.astype(BF)
                else:
                    out[...] = value.astype(BF)
                return carry
            lax.fori_loop(0, count, body, 0)
        return run

    def rs_round(r):
        def half_a1(c, n):
            return G.at[n, r, core, c, :, 0:64]

        def half_b1(c, n):
            return G.at[c // 2, r, core, 2 * n:2 * n + 2, c % 2, 64:128]

        a1 = (z1.at[r, 0, 0], z1.at[r, 0, 1], lambda n: z2.at[r, 0, 0, n], lambda n: z2.at[r, 0, 1, n])
        b1 = (z1.at[r, 1, 0], z1.at[r, 1, 1], lambda n: z2.at[r, 1, 0, n], lambda n: z2.at[r, 1, 1, n])
        yield from zipped([
            rs_ring(half_a1, a1, z, to_zp, to_zm, add_flat((2,)), lambda n: half_a1(z, n)),
            rs_ring(half_b1, b1, y, to_yp, to_ym, add_flat((2,)), lambda n: half_b1(y, n)),
        ])

        def half_a2(c, n):
            return G.at[c // 2, r, core, z, c % 2, 32 * n:32 * n + 32]

        def half_b2(c, n):
            return G.at[yh, r, core, c, yl, 64 + 32 * n:96 + 32 * n]

        a2 = (za.at[0, r, 0], za.at[0, r, 1], lambda n: zb.at[0, r, 0, n], lambda n: zb.at[0, r, 1, n])
        b2 = (za.at[1, r, 0], za.at[1, r, 1], lambda n: zb.at[1, r, 0, n], lambda n: zb.at[1, r, 1, n])
        yield from zipped([
            rs_ring(half_a2, a2, y, to_yp, to_ym, add_flat(()), lambda n: half_a2(y, n)),
            rs_ring(half_b2, b2, z, to_zp, to_zm, add_flat(()), lambda n: half_b2(z, n)),
        ])

    hbase = spread(hid, h, loads[2])
    gbase = spread(cot, g, loads[3])
    got(W.at[yh, other, 0, z, yl], own_recv)
    got(W.at[yh, other, 1, z, yl], own_recv + 1)

    def step(task):
        next(task, None)

    def settle():
        for wait in pending:
            wait()
        pending.clear()

    drain(ag_round(0))
    late = ag_round(1)
    step(late)
    settle()
    for d in (1, 3, 2):
        got(h.at[0, (x + 4 - d) % 4], hbase + d)
    fw = forward(0)
    for _ in fw:
        step(late)
    drain(late)
    settle()
    for l in range(1, 4):
        drain(forward(l))
    for d in (1, 3, 2):
        got(g.at[4, (x + 4 - d) % 4], gbase + d)
    for l in (3, 2, 1):
        drain(backward(l))
    merge(3)
    merge(1)
    early = rs_round(1)
    step(early)
    for _ in backward(0):
        step(early)
    drain(early)
    merge(2)
    merge(0)
    drain(rs_round(0))
    last = sem("r")
    push(G.at[yh, other, core, z, yl], gw.at[core], last, partner)
    gw_ref[core] = G[yh, core, core, z, yl]
    got(gw.at[other], last)
    gw_ref[other] = gw[other]
    for copy in sends:
        copy.wait_send()
    finish_emit()
    assert counters["s"] <= SENDS and counters["r"] <= RECVS and counters["l"] <= 8, counters


SENDS, RECVS = 256, 384


def shards(hidden_in, out_grad, fast_in, fast_out, slow_in, slow_out):
    any_ = pl.BlockSpec(memory_space=pl.ANY)
    so, ig, gw = pl.pallas_call(
        relay,
        out_shape=(
            jax.ShapeDtypeStruct((4, 128, 1024), BF),
            jax.ShapeDtypeStruct((4, 128, 1024), BF),
            jax.ShapeDtypeStruct((2, 128, 1024), BF),
        ),
        in_specs=[any_] * 4,
        out_specs=(any_, any_, pl.BlockSpec(memory_space=pltpu.VMEM)),
        scratch_shapes=[
            pltpu.VMEM((128, 1024), F32),
            pltpu.VMEM((1024, 128), F32),
            pltpu.VMEM((32, 4096), BF),
            pltpu.VMEM((32, 4096), BF),
            pltpu.VMEM((2, 4, 32, 1024), BF),
            pltpu.VMEM((2, 2, 2, 4, 2, 128, 1024), BF),
            pltpu.VMEM((2, 2, 2, 4, 2, 128, 1024), BF),
            pltpu.VMEM((2, 2, 4, 2, 128, 1024), BF),
            pltpu.VMEM((5, 4, 32, 1024), BF),
            pltpu.VMEM((5, 4, 32, 1024), BF),
            pltpu.VMEM((8, 4, 32, 1024 + EXT), BF),
            pltpu.VMEM((8, 4, 32, 1024 + EXT), BF),
            pltpu.VMEM((4, 4, 32, 1024), BF),
            pltpu.VMEM((4, 4, 32, 1024 + EXT), BF),
            pltpu.VMEM((4, 32, 1024), F32),
            pltpu.VMEM((4, 32, EXT), F32),
            pltpu.VMEM((2, 2, 2, 2, 64, 1024), BF),
            pltpu.VMEM((2, 2, 2, 2, 2, 64, 1024), BF),
            pltpu.VMEM((2, 2, 2, 32, 1024), BF),
            pltpu.VMEM((2, 2, 2, 2, 32, 1024), BF),
            pltpu.VMEM((2, 128, 1024), BF),
            pltpu.SemaphoreType.DMA((12,)),
            pltpu.SemaphoreType.DMA((SENDS,)),
            pltpu.SemaphoreType.DMA((RECVS,)),
        ],
        compiler_params=pltpu.CompilerParams(
            collective_id=0, has_side_effects=True, vmem_limit_bytes=67043328
        ),
        name="relay",
    )(hidden_in, out_grad, fast_in, fast_out)

    def whole(pieces):
        return pieces.reshape(4, 128, 4, 256).transpose(1, 2, 0, 3).reshape(1, 128, 4096)

    def synced(fast, slow, grad):
        fresh = fast - RATE * grad
        return slow + MIX * (fresh - slow)

    grad_in = gw[0].astype(F32)
    grad_out = gw[1].astype(F32).T
    return (
        whole(so), whole(ig),
        synced(fast_in, slow_in, grad_in[None]),
        synced(fast_out, slow_out, grad_out[None]),
    )


def solution(mesh):
    placed = (
        P("fsdp", None), P("fsdp", None),
        P("section", "fsdp", None), P("section", None, "fsdp"),
        P("section", "fsdp", None), P("section", None, "fsdp"),
    )
    return jax.shard_map(
        shards, mesh=mesh, in_specs=placed,
        out_specs=(
            P("section", "fsdp", None), P("section", "fsdp", None),
            P("section", "fsdp", None), P("section", None, "fsdp"),
        ),
        check_vma=False,
    )
```

```python
import functools
import math

import jax
import jax.numpy as jnp
from jax import lax
from jax.experimental import pallas as pl
from jax.experimental.pallas import tpu as pltpu
from jax.sharding import PartitionSpec as P

EPS = 1e-05
RATE = 0.5
MIX = 0.5
MESH = pl.DeviceIdType.MESH
BF = jnp.bfloat16
F32 = jnp.float32
EXT = 128


def split_lanes(column):
    high = column.astype(BF)
    low = (column - high.astype(F32)).astype(BF)
    lane = lax.broadcasted_iota(jnp.int32, (column.shape[0], EXT), 1)
    return jnp.where(lane < EXT // 2, high.astype(F32), low.astype(F32)).astype(BF)


def join_lanes(lanes):
    return jnp.sum(lanes.astype(F32), axis=-1, keepdims=True) * (2.0 / EXT)


def relay(
    hid_hbm, cot_hbm, fin_hbm, fout_hbm,
    so_hbm, ig_hbm, gw_ref,
    fin, fout, hid, cot, stage0, own, W, G, Gx, h, g, stg, land, act, pgb, pre, rinv,
    z1, z2, za, zb, gw,
    in_sem, s_send, s_recv,
):
    D, LAT = 4096, 1024
    in_scale, out_scale = 1.0 / math.sqrt(D), 1.0 / math.sqrt(LAT)
    s = lax.axis_index("section")
    f = lax.axis_index("fsdp")
    core, yh = s % 2, s // 2
    z, x, yl = f // 8, (f // 2) % 4, f % 2
    y = yh * 2 + yl
    other = 1 - core

    def dev(yy, zz, xx, cc):
        return ((yy // 2) * 2 + cc, zz * 8 + xx * 2 + yy % 2)

    counters = {"s": 0, "r": 0}
    sends = []

    def sem(kind, n=1):
        at = counters[kind]
        counters[kind] += n
        return at

    def push(src, dst, recv_index, to):
        copy = pltpu.make_async_remote_copy(
            src_ref=src, dst_ref=dst, send_sem=s_send.at[sem("s")], recv_sem=s_recv.at[recv_index],
            device_id=to, device_id_type=MESH,
        )
        copy.start()
        sends.append(copy)

    def got(dst, recv_index):
        pltpu.make_async_remote_copy(
            src_ref=dst, dst_ref=dst, send_sem=s_send.at[0], recv_sem=s_recv.at[recv_index],
            device_id=(s, f), device_id_type=MESH,
        ).wait_recv()

    rows = pl.ds(pl.multiple_of(s * 32, 32), 32)
    loads = [
        pltpu.make_async_copy(fin_hbm.at[0], fin, in_sem.at[0]),
        pltpu.make_async_copy(fout_hbm.at[0], fout, in_sem.at[1]),
        pltpu.make_async_copy(hid_hbm.at[rows], hid, in_sem.at[2]),
        pltpu.make_async_copy(cot_hbm.at[rows], cot, in_sem.at[3]),
    ]
    for c in loads:
        c.start()

    yp, ym, zp, zm = (y + 1) % 4, (y + 3) % 4, (z + 1) % 4, (z + 3) % 4
    to_yp, to_ym = dev(yp, z, x, core), dev(ym, z, x, core)
    to_zp, to_zm = dev(y, zp, x, core), dev(y, zm, x, core)
    partner = dev(y, z, x, other)
    barrier = pltpu.get_barrier_semaphore()
    greeted = [to_yp, to_ym, to_zp, to_zm]
    for ds in range(4):
        for dx in range(4):
            if ds or dx:
                greeted.append(((s + ds) % 4, z * 8 + ((x + dx) % 4) * 2 + yl))
    for to in greeted:
        pl.semaphore_signal(barrier, inc=1, device_id=to, device_id_type=MESH)
    pl.semaphore_wait(barrier, len(greeted))

    def xdev(d):
        return (s, z * 8 + ((x + d) % 4) * 2 + yl)

    def quarters(rows):
        return rows.astype(BF).reshape(2, 2, 32, LAT)

    mates = sem("r", 8)

    def share():
        loads[0].wait()
        own[0] = quarters(fin[...] * in_scale)
        loads[1].wait()
        own[1] = quarters((fout[...] * out_scale).T)
        for c in range(2):
            push(own.at[c, 1 - yh], W.at[s, c, z, yl, 1 - yh], mates + core, ((1 - yh) * 2 + c, f))
        push(own.at[:, yh], W.at[s, :, z, yl, yh], mates + 2, partner)
        W[s, 0, z, yl, yh] = own[0, yh]
        W[s, 1, z, yl, yh] = own[1, yh]

    def shared():
        far = pl.ds(2 * (1 - yh), 2)
        for c in range(2):
            got(W.at[2 * (1 - yh) + c, core, z, yl, yh], mates + c)
        push(W.at[far, core, z, yl, yh], W.at[far, core, z, yl, yh], mates + 3, partner)
        got(W.at[yh * 2 + other, :, z, yl, yh], mates + 2)
        pending.append((0, lambda: got(W.at[far, other, z, yl, yh], mates + 3)))

    def spread(source, target, load):
        load.wait()
        base = sem("r", 4)
        slot = 0 if target is h else 1
        for xx in range(4):
            for zz in range(4):
                stage0[slot, xx, :, zz * 256:(zz + 1) * 256] = source[:, zz * 1024 + xx * 256: zz * 1024 + (xx + 1) * 256]
        level = 0 if target is h else 4
        target[level, x] = stage0[slot, x]
        for d in (1, 3, 2):
            push(stage0.at[slot, (x + d) % 4], target.at[level, x], base + d, xdev(d))
        return base

    def ag_ring(item, half, q, to_plus, to_minus, level):
        base = sem("r", 8)
        qp, qm, qo = (q + 1) % 4, (q + 3) % 4, (q + 2) % 4
        push(item(q), item(q), base + 0, to_plus)
        push(item(q), item(q), base + 1, to_minus)
        yield
        got(item(qm), base + 0)
        push(half(qm, 0), half(qm, 0), base + 2, to_plus)
        got(item(qp), base + 1)
        push(half(qp, 1), half(qp, 1), base + 3, to_minus)
        push(item(qm), item(qm), base + 4, partner)
        push(item(qp), item(qp), base + 5, partner)
        yield
        got(half(qo, 0), base + 2)
        push(half(qo, 0), half(qo, 0), base + 6, partner)
        got(half(qo, 1), base + 3)
        push(half(qo, 1), half(qo, 1), base + 7, partner)
        pending.append((level, lambda: twin(item, half, q, base)))

    pending = []

    def twin(item, half, q, base):
        qp, qm, qo = (q + 1) % 4, (q + 3) % 4, (q + 2) % 4
        got(item(qm, other), base + 4)
        got(item(qp, other), base + 5)
        got(half(qo, 0, other), base + 6)
        got(half(qo, 1, other), base + 7)

    def settle(level):
        for entry in list(pending):
            if entry[0] <= level:
                entry[1]()
                pending.remove(entry)

    def gather_first(ls, level):
        def item_a(c, k=core):
            return W.at[ls, k, z, c % 2, c // 2, 0]

        def half_a(c, n, k=core):
            return W.at[ls, k, z, c % 2, c // 2, 0, 16 * n:16 * n + 16]

        def item_b(c, k=core):
            return W.at[ls, k, c, yl, yh, 1]

        def half_b(c, n, k=core):
            return W.at[ls, k, c, yl, yh, 1, 16 * n:16 * n + 16]

        return zipped([
            ag_ring(item_a, half_a, y, to_yp, to_ym, level), ag_ring(item_b, half_b, z, to_zp, to_zm, level)])

    def gather_second(l):
        def item_a(c, k=core):
            return W.at[l, k, c, :, :, 0]

        def half_a(c, n, k=core):
            return W.at[l, k, c, n, :, 0]

        def item_b(c, k=core):
            return W.at[l, k, :, c % 2, c // 2, 1]

        def half_b(c, n, k=core):
            return W.at[l, k, 2 * n:2 * n + 2, c % 2, c // 2, 1]

        return zipped([
            ag_ring(item_a, half_a, z, to_zp, to_zm, l), ag_ring(item_b, half_b, y, to_yp, to_ym, l)])

    def zipped(tasks):
        tasks = list(tasks)
        while tasks:
            tasks = [t for t in tasks if next(t, True) is not True]
            if tasks:
                yield

    def drain(task):
        for _ in task:
            pass

    def dot_nn(a, b):
        return lax.dot_general(a, b, (((1,), (0,)), ((), ())), preferred_element_type=F32)

    def dot_nt(a, b):
        return lax.dot_general(a, b, (((1,), (1,)), ((), ())), preferred_element_type=F32)

    def dot_tn(a, b):
        return lax.dot_general(a, b, (((0,), (0,)), ((), ())), preferred_element_type=F32)

    NT = 256

    def project(source, level, l, k, step):
        left = source[level].reshape(128, 1024)

        def body(i, carry):
            c = pl.multiple_of(i * NT, NT)
            right = W[l, k, :, :, :, :, :, pl.ds(c, NT)].reshape(1024, NT)
            stg[step, :, :, pl.ds(c, NT)] = dot_nn(left, right).astype(BF).reshape(4, 32, NT)
            return carry
        lax.fori_loop(0, LAT // NT, body, 0)

    def scatter(step):
        base = sem("r", 4)
        land[step, x] = stg[step, x]
        for d in (2, 1, 3):
            push(stg.at[step, (x + d) % 4], land.at[step, x], base + d, xdev(d))
        return base

    def summed(step, base):
        for d in (1, 3, 2):
            got(land.at[step, (x + 4 - d) % 4], base + d)

    def broadcast(buf, l):
        base = sem("r", 4)
        for d in (2, 1, 3):
            push(buf.at[l, x], buf.at[l, x], base + d, xdev(d))
        return base

    def collect(buf, l, base):
        for d in (1, 3, 2):
            got(buf.at[l, (x + 4 - d) % 4], base + d)

    def emit(source, level, l, out_ref):
        base = sem("r", 16)
        emitted.append((l, base, out_ref))

        def part(ds):
            for d in ds:
                src = source.at[level, (x + d) % 4]
                dst = out_ref.at[x, rows]
                to = (l, z * 8 + ((x + d) % 4) * 2 + yl)
                copy = pltpu.make_async_remote_copy(
                    src_ref=src, dst_ref=dst, send_sem=s_send.at[sem("s")], recv_sem=s_recv.at[base + s * 4 + x],
                    device_id=to, device_id_type=MESH,
                )
                if d:
                    copy.start()
                    sends.append(copy)
                else:
                    local = pltpu.make_async_copy(src, dst, in_sem.at[4 + sem("l")])

                    @pl.when(s != l)
                    def _():
                        copy.start()

                    @pl.when(s == l)
                    def _():
                        local.start()
                    locals_.append((l, copy, local))
        parts_due.append(lambda: part((0, 2)))
        parts_due.append(lambda: part((1, 3)))

    parts_due = []

    def emit_next():
        if parts_due:
            parts_due.pop(0)()

    counters["l"] = 0
    locals_, emitted = [], []

    def finish_emit():
        for l, copy, local in locals_:
            @pl.when(s != l)
            def _():
                copy.wait_send()

            @pl.when(s == l)
            def _():
                local.wait()
        for l, base, out_ref in emitted:
            @pl.when(s == l)
            def _():
                for ds in range(4):
                    for dx in range(4):
                        if ds or dx:
                            ss, xx = (s + ds) % 4, (x + dx) % 4
                            got(out_ref.at[xx, pl.ds(pl.multiple_of(ss * 32, 32), 32)], base + ss * 4 + xx)

    def forward(l):
        project(h, l, l, 0, l)
        wide = h[l].reshape(128, 1024).astype(F32)
        ss = jnp.sum(wide * wide, axis=-1, keepdims=True)
        stg[l, :, :, LAT:] = split_lanes(ss).reshape(4, 32, EXT)
        base = scatter(l)
        emit_next()
        yield
        summed(l, base)
        total = land[l, 0].astype(F32)
        for xx in range(1, 4):
            total = total + land[l, xx].astype(F32)
        r = lax.rsqrt(join_lanes(total[:, LAT:]) * (1.0 / D) + EPS)
        v = total[:, :LAT] * r
        pre[l] = v
        rinv[l] = jnp.broadcast_to(r, (32, EXT))
        act[l, x] = (v / (1.0 + jnp.exp(-v))).astype(BF)
        base = broadcast(act, l)
        emit_next()
        yield
        collect(act, l, base)
        left = act[l].reshape(128, 1024)

        def body(i, carry):
            c = pl.multiple_of(i * NT, NT)
            right = W[l, 1, i].reshape(NT, 1024)
            old = h[l, :, :, pl.ds(c, NT)].reshape(128, NT).astype(F32)
            h[l + 1, :, :, pl.ds(c, NT)] = (old + dot_nt(left, right)).astype(BF).reshape(4, 32, NT)
            return carry
        lax.fori_loop(0, 4, body, 0)
        emit(h, l + 1, l, so_hbm)

    def wgrad(l, kind, left_ref, left_level, right_ref, scale):
        right = right_ref[l, :, :, :LAT].reshape(128, LAT)

        def body(i, carry):
            c = pl.multiple_of(i * 128, 128)
            left = left_ref[left_level, :, :, pl.ds(c, 128)].reshape(128, 128)
            value = (dot_tn(left, right) * scale).astype(BF)
            G[l, kind, i // 2, i % 2] = value.reshape(2, 2, 32, LAT)
            return carry
        lax.fori_loop(0, 8, body, 0)

    def backward(l):
        step = 7 - l
        project(g, l + 1, l, 1, step)
        base = scatter(step)
        emit_next()
        if l < 3:
            input_grads(l + 1)
        yield
        summed(step, base)
        total = land[step, 0, :, :LAT].astype(F32)
        for xx in range(1, 4):
            total = total + land[step, xx, :, :LAT].astype(F32)
        v = pre[l]
        r = rinv[l][:, :1]
        sg = 1.0 / (1.0 + jnp.exp(-v))
        scaled = (r * (total * sg * (1.0 + v * (1.0 - sg)))).astype(BF)
        kappa = r * jnp.sum(scaled.astype(F32) * v, axis=-1, keepdims=True) * (1.0 / D)
        pgb[l, x, :, :LAT] = scaled
        pgb[l, x, :, LAT:] = split_lanes(kappa)
        base = broadcast(pgb, l)
        emit_next()
        wgrad(l, 1, g, l + 1, act, out_scale)
        yield
        collect(pgb, l, base)
        left = pgb[l, :, :, :LAT].reshape(128, LAT)
        kap = join_lanes(pgb[l, :, :, LAT:].reshape(128, EXT))

        if l == 0:
            input_grads(0)

        def body(i, carry):
            c = pl.multiple_of(i * NT, NT)
            right = W[l, 0, i].reshape(NT, 1024)
            old = g[l + 1, :, :, pl.ds(c, NT)].reshape(128, NT).astype(F32)
            base_h = h[l, :, :, pl.ds(c, NT)].reshape(128, NT).astype(F32)
            g[l, :, :, pl.ds(c, NT)] = (old + dot_nt(left, right) - base_h * kap).astype(BF).reshape(4, 32, NT)
            return carry
        lax.fori_loop(0, 4, body, 0)
        emit(g, l, l, ig_hbm)

    def input_grads(l):
        wgrad(l, 0, h, l, pgb, in_scale)
        gx_base[l] = sem("r")
        push(G.at[l, other], Gx.at[l], gx_base[l], partner)

    gx_base = {}

    def merge(l):
        got(Gx.at[l], gx_base[l])

        def body(i, carry):
            at = (l, core, i // 2, i % 2)
            G[at] = G[at] + Gx[l, i // 2, i % 2]
            return carry
        lax.fori_loop(0, 8, body, 0)

    def rs_ring(half, lands, q, to_plus, to_minus, parts, result):
        p1, m1, p2, m2 = lands
        base = sem("r", 6)
        qp, qm, qo = (q + 1) % 4, (q + 3) % 4, (q + 2) % 4
        push(half(qo, 0), p1, base + 0, to_plus)
        push(half(qo, 1), m1, base + 1, to_minus)
        push(half(qp, 1), p2(1), base + 2, to_plus)
        push(half(qm, 0), m2(0), base + 3, to_minus)
        yield
        got(p1, base + 0)
        parts(half(qp, 0), half(qp, 0), [p1])
        push(half(qp, 0), p2(0), base + 4, to_plus)
        got(m1, base + 1)
        parts(half(qm, 1), half(qm, 1), [m1])
        push(half(qm, 1), m2(1), base + 5, to_minus)
        yield
        got(m2(0), base + 3)
        got(p2(0), base + 4)
        parts(half(q, 0), result(0), [p2(0), m2(0)])
        got(p2(1), base + 2)
        got(m2(1), base + 5)
        parts(half(q, 1), result(1), [p2(1), m2(1)])

    def add_flat(shape):
        count = math.prod(shape)

        def run(own, out, terms):
            def body(i, carry):
                index, rest = [], i
                for n in reversed(shape):
                    index.insert(0, rest % n)
                    rest = rest // n
                index = tuple(index)
                value = own[index] if index else own[...]
                value = value.astype(F32)
                for t in terms:
                    value = value + (t[index] if index else t[...]).astype(F32)
                if index:
                    out[index] = value.astype(BF)
                else:
                    out[...] = value.astype(BF)
                return carry
            lax.fori_loop(0, count, body, 0)
        return run

    def reduce_round(l):
        def half_a1(c, n):
            return G.at[l, core, c, n, :, 0]

        def half_b1(c, n):
            return G.at[l, core, 2 * n:2 * n + 2, c % 2, c // 2, 1]

        a1 = (z1.at[l, 0, 0], z1.at[l, 0, 1], lambda n: z2.at[l, 0, 0, n], lambda n: z2.at[l, 0, 1, n])
        b1 = (z1.at[l, 1, 0], z1.at[l, 1, 1], lambda n: z2.at[l, 1, 0, n], lambda n: z2.at[l, 1, 1, n])
        yield from zipped([
            rs_ring(half_a1, a1, z, to_zp, to_zm, add_flat((2,)), lambda n: half_a1(z, n)),
            rs_ring(half_b1, b1, y, to_yp, to_ym, add_flat((2,)), lambda n: half_b1(y, n)),
        ])

        def half_a2(c, n):
            return G.at[l, core, z, c % 2, c // 2, 0, 16 * n:16 * n + 16]

        def half_b2(c, n):
            return G.at[l, core, c, yl, yh, 1, 16 * n:16 * n + 16]

        a2 = (za.at[l, 0, 0], za.at[l, 0, 1], lambda n: zb.at[l, 0, 0, n], lambda n: zb.at[l, 0, 1, n])
        b2 = (za.at[l, 1, 0], za.at[l, 1, 1], lambda n: zb.at[l, 1, 0, n], lambda n: zb.at[l, 1, 1, n])
        yield from zipped([
            rs_ring(half_a2, a2, y, to_yp, to_ym, add_flat(()), lambda n: half_a2(y, n)),
            rs_ring(half_b2, b2, z, to_zp, to_zm, add_flat(()), lambda n: half_b2(z, n)),
        ])
        mine = G.at[l, core, z, yl, yh]
        copy = pltpu.make_async_remote_copy(
            src_ref=mine, dst_ref=gw.at[core, yh], send_sem=s_send.at[sem("s")], recv_sem=s_recv.at[home + s],
            device_id=(l, f), device_id_type=MESH,
        )

        @pl.when(s != l)
        def _():
            copy.start()

        @pl.when(s == l)
        def _():
            gw[core, yh] = mine[...]
        sent_home.append((l, copy))

    home = sem("r", 4)
    sent_home = []

    def step(task, n=1):
        for _ in range(n):
            next(task, None)

    share()
    hbase = spread(hid, h, loads[2])
    gbase = spread(cot, g, loads[3])
    shared()
    ready = set()

    def gather():
        first, rest = gather_first(0, 0), gather_first(slice(1, 4), 1)
        step(first)
        step(rest)
        yield
        yield from first
        current = gather_second(0)
        step(current)
        yield from rest
        for l in range(4):
            step(current)
            following = gather_second(l + 1) if l < 3 else None
            if following is not None:
                step(following)
            yield
            drain(current)
            ready.add(l)
            yield
            current = following

    bulk = gather()

    def need(l):
        while l not in ready:
            step(bulk)
        settle(l)

    need(0)
    for d in (1, 3, 2):
        got(h.at[0, (x + 4 - d) % 4], hbase + d)
    for l in range(4):
        need(l)
        for _ in forward(l):
            step(bulk)
    for d in (1, 3, 2):
        got(g.at[4, (x + 4 - d) % 4], gbase + d)
    running = []
    for l in (3, 2, 1, 0):
        for n, _ in enumerate(backward(l)):
            for task in running:
                step(task)
            if n == 1 and l < 3:
                merge(l + 1)
                running.append(reduce_round(l + 1))
                step(running[-1])
    while parts_due:
        emit_next()
    for task in running:
        step(task)
    merge(0)
    running.append(reduce_round(0))
    drain(zipped(running))
    for l, copy in sent_home:
        @pl.when(s != l)
        def _():
            copy.wait_send()
    for ds in range(1, 4):
        ss = (s + ds) % 4
        got(gw.at[ss % 2, ss // 2], home + ss)
    gw_ref[...] = gw[...].reshape(2, 128, LAT)
    for copy in sends:
        copy.wait_send()
    finish_emit()
    assert counters["s"] <= SENDS and counters["r"] <= RECVS and counters["l"] <= 8, counters


SENDS, RECVS = 352, 480


def shards(hidden_in, out_grad, fast_in, fast_out, slow_in, slow_out):
    any_ = pl.BlockSpec(memory_space=pl.ANY)
    so, ig, gw = pl.pallas_call(
        relay,
        out_shape=(
            jax.ShapeDtypeStruct((4, 128, 1024), BF),
            jax.ShapeDtypeStruct((4, 128, 1024), BF),
            jax.ShapeDtypeStruct((2, 128, 1024), BF),
        ),
        in_specs=[any_] * 4,
        out_specs=(any_, any_, pl.BlockSpec(memory_space=pltpu.VMEM)),
        scratch_shapes=[
            pltpu.VMEM((128, 1024), F32),
            pltpu.VMEM((1024, 128), F32),
            pltpu.VMEM((32, 4096), BF),
            pltpu.VMEM((32, 4096), BF),
            pltpu.VMEM((2, 4, 32, 1024), BF),
            pltpu.VMEM((2, 2, 2, 32, 1024), BF),
            pltpu.VMEM((4, 2, 4, 2, 2, 2, 32, 1024), BF),
            pltpu.VMEM((4, 2, 4, 2, 2, 2, 32, 1024), BF),
            pltpu.VMEM((4, 4, 2, 2, 2, 32, 1024), BF),
            pltpu.VMEM((5, 4, 32, 1024), BF),
            pltpu.VMEM((5, 4, 32, 1024), BF),
            pltpu.VMEM((8, 4, 32, 1024 + EXT), BF),
            pltpu.VMEM((8, 4, 32, 1024 + EXT), BF),
            pltpu.VMEM((4, 4, 32, 1024), BF),
            pltpu.VMEM((4, 4, 32, 1024 + EXT), BF),
            pltpu.VMEM((4, 32, 1024), F32),
            pltpu.VMEM((4, 32, EXT), F32),
            pltpu.VMEM((4, 2, 2, 2, 32, 1024), BF),
            pltpu.VMEM((4, 2, 2, 2, 2, 32, 1024), BF),
            pltpu.VMEM((4, 2, 2, 16, 1024), BF),
            pltpu.VMEM((4, 2, 2, 2, 16, 1024), BF),
            pltpu.VMEM((2, 2, 2, 32, 1024), BF),
            pltpu.SemaphoreType.DMA((12,)),
            pltpu.SemaphoreType.DMA((SENDS,)),
            pltpu.SemaphoreType.DMA((RECVS,)),
        ],
        compiler_params=pltpu.CompilerParams(
            collective_id=0, has_side_effects=True, vmem_limit_bytes=67043328
        ),
        name="relay",
    )(hidden_in, out_grad, fast_in, fast_out)

    return pl.pallas_call(
        finish,
        out_shape=(
            jax.ShapeDtypeStruct((1, 128, 4096), BF),
            jax.ShapeDtypeStruct((1, 128, 4096), BF),
            jax.ShapeDtypeStruct((1, 128, 1024), F32),
            jax.ShapeDtypeStruct((1, 1024, 128), F32),
        ),
        in_specs=[any_] * 7,
        out_specs=(any_,) * 4,
        scratch_shapes=[
            pltpu.VMEM((2, 4, 128, 1024), BF),
            pltpu.VMEM((2, 128, 1024), BF),
            pltpu.VMEM((2, 128, 1024), F32),
            pltpu.VMEM((2, 1024, 128), F32),
            pltpu.VMEM((128, 1024), F32),
            pltpu.VMEM((1024, 128), F32),
            pltpu.SemaphoreType.DMA((16,)),
            pltpu.SemaphoreType.DMA((40,)),
        ],
        name="finish",
    )(so, ig, gw, fast_in, fast_out, slow_in, slow_out)


def finish(so, ig, gw, fi, fo, si, so_slow, o0, o1, o2, o3, acts, grads, wi, wo, ri, ro, insem, outsem):
    loads = []

    def load(src, dst):
        c = pltpu.make_async_copy(src, dst, insem.at[len(loads)])
        c.start()
        loads.append(c)
        return c

    weights = [load(gw, grads), load(fo.at[0], wo.at[0]), load(so_slow.at[0], wo.at[1]),
               load(fi.at[0], wi.at[0]), load(si.at[0], wi.at[1])]
    pieces = [[load(t.at[x], acts.at[k, x]) for x in range(4)] for k, t in enumerate((so, ig))]
    stores = []

    def store(src, dst):
        c = pltpu.make_async_copy(src, dst, outsem.at[len(stores)])
        c.start()
        stores.append(c)

    for k, out in enumerate((o0, o1)):
        for x in range(4):
            pieces[k][x].wait()
            for zz in range(4):
                at = zz * 1024 + x * 256
                store(acts.at[k, x, :, zz * 256:(zz + 1) * 256], out.at[0, :, at:at + 256])

    def synced(fast, slow, grad):
        return slow + MIX * ((fast - RATE * grad) - slow)

    for c in weights[:3]:
        c.wait()
    ro[...] = synced(wo[0], wo[1], grads[1].astype(F32).T)
    store(ro, o3.at[0])
    for c in weights[3:]:
        c.wait()
    ri[...] = synced(wi[0], wi[1], grads[0].astype(F32))
    store(ri, o2.at[0])
    for c in stores:
        c.wait()


def solution(mesh):
    placed = (
        P("fsdp", None), P("fsdp", None),
        P("section", "fsdp", None), P("section", None, "fsdp"),
        P("section", "fsdp", None), P("section", None, "fsdp"),
    )
    return jax.shard_map(
        shards, mesh=mesh, in_specs=placed,
        out_specs=(
            P("section", "fsdp", None), P("section", "fsdp", None),
            P("section", "fsdp", None), P("section", None, "fsdp"),
        ),
        check_vma=False,
    )
```

```python
import functools
import math

import jax
import jax.numpy as jnp
from jax import lax
from jax.experimental import pallas as pl
from jax.experimental.pallas import tpu as pltpu
from jax.sharding import PartitionSpec as P

EPS = 1e-05
RATE = 0.5
MIX = 0.5
MESH = pl.DeviceIdType.MESH
BF = jnp.bfloat16
F32 = jnp.float32
EXT = 128


def split_lanes(column):
    high = column.astype(BF)
    low = (column - high.astype(F32)).astype(BF)
    lane = lax.broadcasted_iota(jnp.int32, (column.shape[0], EXT), 1)
    return jnp.where(lane < EXT // 2, high.astype(F32), low.astype(F32)).astype(BF)


def join_lanes(lanes):
    return jnp.sum(lanes.astype(F32), axis=-1, keepdims=True) * (2.0 / EXT)


def relay(
    hid_hbm, cot_hbm, fin_hbm, fout_hbm,
    so_hbm, ig_hbm, gw_ref,
    fin, fout, hid, cot, stage0, own, W, G, Gx, h, g, stg, land, act, pgb, pre, rinv,
    z1, z2, za, zb, gw,
    in_sem, s_send, s_recv,
):
    D, LAT = 4096, 1024
    in_scale, out_scale = 1.0 / math.sqrt(D), 1.0 / math.sqrt(LAT)
    s = lax.axis_index("section")
    f = lax.axis_index("fsdp")
    core, yh = s % 2, s // 2
    z, x, yl = f // 8, (f // 2) % 4, f % 2
    y = yh * 2 + yl
    other = 1 - core

    def dev(yy, zz, xx, cc):
        return ((yy // 2) * 2 + cc, zz * 8 + xx * 2 + yy % 2)

    counters = {"s": 0, "r": 0}
    sends = []

    def sem(kind, n=1):
        at = counters[kind]
        counters[kind] += n
        return at

    def push(src, dst, recv_index, to):
        copy = pltpu.make_async_remote_copy(
            src_ref=src, dst_ref=dst, send_sem=s_send.at[sem("s")], recv_sem=s_recv.at[recv_index],
            device_id=to, device_id_type=MESH,
        )
        copy.start()
        sends.append(copy)

    def got(dst, recv_index):
        pltpu.make_async_remote_copy(
            src_ref=dst, dst_ref=dst, send_sem=s_send.at[0], recv_sem=s_recv.at[recv_index],
            device_id=(s, f), device_id_type=MESH,
        ).wait_recv()

    rows = pl.ds(pl.multiple_of(s * 32, 32), 32)
    loads = [
        pltpu.make_async_copy(fin_hbm.at[0], fin, in_sem.at[0]),
        pltpu.make_async_copy(fout_hbm.at[0], fout, in_sem.at[1]),
        pltpu.make_async_copy(hid_hbm.at[rows], hid, in_sem.at[2]),
        pltpu.make_async_copy(cot_hbm.at[rows], cot, in_sem.at[3]),
    ]
    for c in loads:
        c.start()

    yp, ym, zp, zm = (y + 1) % 4, (y + 3) % 4, (z + 1) % 4, (z + 3) % 4
    to_yp, to_ym = dev(yp, z, x, core), dev(ym, z, x, core)
    to_zp, to_zm = dev(y, zp, x, core), dev(y, zm, x, core)
    partner = dev(y, z, x, other)
    barrier = pltpu.get_barrier_semaphore()
    greeted = [to_yp, to_ym, to_zp, to_zm]
    for ds in range(4):
        for dx in range(4):
            if ds or dx:
                greeted.append(((s + ds) % 4, z * 8 + ((x + dx) % 4) * 2 + yl))
    for to in greeted:
        pl.semaphore_signal(barrier, inc=1, device_id=to, device_id_type=MESH)
    pl.semaphore_wait(barrier, len(greeted))

    def xdev(d):
        return (s, z * 8 + ((x + d) % 4) * 2 + yl)

    def quarters(rows):
        return rows.astype(BF).reshape(2, 2, 32, LAT)

    mates = sem("r", 8)

    def share():
        for c, value in ((0, lambda: fin[...] * in_scale), (1, lambda: (fout[...] * out_scale).T)):
            loads[c].wait()
            own[c] = quarters(value())
            push(own.at[c, 1 - yh], W.at[s, c, z, yl, 1 - yh], mates + core, ((1 - yh) * 2 + c, f))
        push(own.at[:, yh], W.at[s, :, z, yl, yh], mates + 2, partner)
        W[s, 0, z, yl, yh] = own[0, yh]
        W[s, 1, z, yl, yh] = own[1, yh]

    def shared():
        far = pl.ds(2 * (1 - yh), 2)
        for c in range(2):
            got(W.at[2 * (1 - yh) + c, core, z, yl, yh], mates + c)
        push(W.at[far, core, z, yl, yh], W.at[far, core, z, yl, yh], mates + 3, partner)
        got(W.at[yh * 2 + other, :, z, yl, yh], mates + 2)
        pending.append((0, lambda: got(W.at[far, other, z, yl, yh], mates + 3)))

    def spread(source, target, load):
        load.wait()
        base = sem("r", 4)
        slot = 0 if target is h else 1
        for xx in range(4):
            for zz in range(4):
                stage0[slot, xx, :, zz * 256:(zz + 1) * 256] = source[:, zz * 1024 + xx * 256: zz * 1024 + (xx + 1) * 256]
        level = 0 if target is h else 4
        target[level, x] = stage0[slot, x]
        for d in (1, 3, 2):
            push(stage0.at[slot, (x + d) % 4], target.at[level, x], base + d, xdev(d))
        return base

    def ag_ring(item, half, q, to_plus, to_minus, level):
        base = sem("r", 10)
        qp, qm, qo = (q + 1) % 4, (q + 3) % 4, (q + 2) % 4
        push(half(q, 0), half(q, 0), base + 0, to_plus)
        push(half(q, 1), half(q, 1), base + 1, to_minus)
        push(half(q, 1), half(q, 1), base + 2, to_plus)
        push(half(q, 0), half(q, 0), base + 3, to_minus)
        yield
        got(half(qm, 0), base + 0)
        push(half(qm, 0), half(qm, 0), base + 4, to_plus)
        got(half(qp, 1), base + 1)
        push(half(qp, 1), half(qp, 1), base + 5, to_minus)
        got(half(qm, 1), base + 2)
        push(item(qm), item(qm), base + 6, partner)
        got(half(qp, 0), base + 3)
        push(item(qp), item(qp), base + 7, partner)
        yield
        got(half(qo, 0), base + 4)
        push(half(qo, 0), half(qo, 0), base + 8, partner)
        got(half(qo, 1), base + 5)
        push(half(qo, 1), half(qo, 1), base + 9, partner)
        pending.append((level, lambda: twin(item, half, q, base)))

    pending = []

    def twin(item, half, q, base):
        qp, qm, qo = (q + 1) % 4, (q + 3) % 4, (q + 2) % 4
        got(item(qm, other), base + 6)
        got(item(qp, other), base + 7)
        got(half(qo, 0, other), base + 8)
        got(half(qo, 1, other), base + 9)

    def settle(level):
        for entry in list(pending):
            if entry[0] <= level:
                entry[1]()
                pending.remove(entry)

    def gather_first(ls, level):
        def item_a(c, k=core):
            return W.at[ls, k, z, c % 2, c // 2, 0]

        def half_a(c, n, k=core):
            return W.at[ls, k, z, c % 2, c // 2, 0, 16 * n:16 * n + 16]

        def item_b(c, k=core):
            return W.at[ls, k, c, yl, yh, 1]

        def half_b(c, n, k=core):
            return W.at[ls, k, c, yl, yh, 1, 16 * n:16 * n + 16]

        return zipped([
            ag_ring(item_a, half_a, y, to_yp, to_ym, level), ag_ring(item_b, half_b, z, to_zp, to_zm, level)])

    def gather_second(l):
        def item_a(c, k=core):
            return W.at[l, k, c, :, :, 0]

        def half_a(c, n, k=core):
            return W.at[l, k, c, n, :, 0]

        def item_b(c, k=core):
            return W.at[l, k, :, c % 2, c // 2, 1]

        def half_b(c, n, k=core):
            return W.at[l, k, 2 * n:2 * n + 2, c % 2, c // 2, 1]

        return zipped([
            ag_ring(item_a, half_a, z, to_zp, to_zm, l), ag_ring(item_b, half_b, y, to_yp, to_ym, l)])

    def zipped(tasks):
        tasks = list(tasks)
        while tasks:
            tasks = [t for t in tasks if next(t, True) is not True]
            if tasks:
                yield

    def drain(task):
        for _ in task:
            pass

    def dot_nn(a, b):
        return lax.dot_general(a, b, (((1,), (0,)), ((), ())), preferred_element_type=F32)

    def dot_nt(a, b):
        return lax.dot_general(a, b, (((1,), (1,)), ((), ())), preferred_element_type=F32)

    def dot_tn(a, b):
        return lax.dot_general(a, b, (((0,), (0,)), ((), ())), preferred_element_type=F32)

    NT = 256

    def project(source, level, l, k, step):
        left = source[level].reshape(128, 1024)

        def body(i, carry):
            c = pl.multiple_of(i * NT, NT)
            right = W[l, k, :, :, :, :, :, pl.ds(c, NT)].reshape(1024, NT)
            stg[step, :, :, pl.ds(c, NT)] = dot_nn(left, right).astype(BF).reshape(4, 32, NT)
            return carry
        lax.fori_loop(0, LAT // NT, body, 0, unroll=True)

    def scatter(step):
        base = sem("r", 4)
        for d in (2, 1, 3):
            push(stg.at[step, (x + d) % 4], land.at[step, x], base + d, xdev(d))
        land[step, x] = stg[step, x]
        return base

    def summed(step, base):
        for d in (1, 3, 2):
            got(land.at[step, (x + 4 - d) % 4], base + d)

    def broadcast(buf, l):
        base = sem("r", 4)
        for d in (2, 1, 3):
            push(buf.at[l, x], buf.at[l, x], base + d, xdev(d))
        return base

    def collect(buf, l, base):
        for d in (1, 3, 2):
            got(buf.at[l, (x + 4 - d) % 4], base + d)

    def emit(source, level, l, out_ref):
        base = sem("r", 16)
        emitted.append((l, base, out_ref))

        def part(ds):
            for d in ds:
                src = source.at[level, (x + d) % 4]
                dst = out_ref.at[x, rows]
                to = (l, z * 8 + ((x + d) % 4) * 2 + yl)
                copy = pltpu.make_async_remote_copy(
                    src_ref=src, dst_ref=dst, send_sem=s_send.at[sem("s")], recv_sem=s_recv.at[base + s * 4 + x],
                    device_id=to, device_id_type=MESH,
                )
                if d:
                    copy.start()
                    sends.append(copy)
                else:
                    local = pltpu.make_async_copy(src, dst, in_sem.at[4 + sem("l")])

                    @pl.when(s != l)
                    def _():
                        copy.start()

                    @pl.when(s == l)
                    def _():
                        local.start()
                    locals_.append((l, copy, local))
        parts_due.append(lambda: part((0, 2)))
        parts_due.append(lambda: part((1, 3)))

    parts_due = []

    def emit_next(last=False):
        counters["w"] += 1
        if parts_due and (last or counters["w"] > EMIT_FROM):
            parts_due.pop(0)()

    counters["l"] = counters["w"] = 0
    locals_, emitted = [], []

    def finish_emit():
        for l, copy, local in locals_:
            @pl.when(s != l)
            def _():
                copy.wait_send()

            @pl.when(s == l)
            def _():
                local.wait()
        for l, base, out_ref in emitted:
            @pl.when(s == l)
            def _():
                for ds in range(4):
                    for dx in range(4):
                        if ds or dx:
                            ss, xx = (s + ds) % 4, (x + dx) % 4
                            got(out_ref.at[xx, pl.ds(pl.multiple_of(ss * 32, 32), 32)], base + ss * 4 + xx)

    def forward(l):
        project(h, l, l, 0, l)
        wide = h[l].reshape(128, 1024).astype(F32)
        ss = jnp.sum(wide * wide, axis=-1, keepdims=True)
        stg[l, :, :, LAT:] = split_lanes(ss).reshape(4, 32, EXT)
        base = scatter(l)
        emit_next()
        yield
        summed(l, base)
        total = land[l, 0].astype(F32)
        for xx in range(1, 4):
            total = total + land[l, xx].astype(F32)
        r = lax.rsqrt(join_lanes(total[:, LAT:]) * (1.0 / D) + EPS)
        v = total[:, :LAT] * r
        act[l, x] = (v / (1.0 + jnp.exp(-v))).astype(BF)
        base = broadcast(act, l)
        pre[l] = v
        rinv[l] = jnp.broadcast_to(r, (32, EXT))
        emit_next()
        yield
        collect(act, l, base)
        left = act[l].reshape(128, 1024)

        def body(i, carry):
            c = pl.multiple_of(i * NT, NT)
            right = W[l, 1, i].reshape(NT, 1024)
            old = h[l, :, :, pl.ds(c, NT)].reshape(128, NT).astype(F32)
            h[l + 1, :, :, pl.ds(c, NT)] = (old + dot_nt(left, right)).astype(BF).reshape(4, 32, NT)
            return carry
        lax.fori_loop(0, 4, body, 0, unroll=True)
        emit(h, l + 1, l, so_hbm)

    def wgrad(l, kind, left_ref, left_level, right_ref, scale):
        right = right_ref[l, :, :, :LAT].reshape(128, LAT)

        def body(i, carry):
            c = pl.multiple_of(i * 128, 128)
            left = left_ref[left_level, :, :, pl.ds(c, 128)].reshape(128, 128)
            value = (dot_tn(left, right) * scale).astype(BF)
            G[l, kind, i // 2, i % 2] = value.reshape(2, 2, 32, LAT)
            return carry
        lax.fori_loop(0, 8, body, 0, unroll=4)

    begun = {}

    def begin(l):
        project(g, l + 1, l, 1, 7 - l)
        begun[l] = scatter(7 - l)

    def backward(l):
        step = 7 - l
        if l not in begun:
            begin(l)
        base = begun[l]
        emit_next()
        if 1 < l + 1 < 4 and l > 0:
            input_grads(l + 1)
        yield
        summed(step, base)
        total = land[step, 0, :, :LAT].astype(F32)
        for xx in range(1, 4):
            total = total + land[step, xx, :, :LAT].astype(F32)
        v = pre[l]
        r = rinv[l][:, :1]
        sg = 1.0 / (1.0 + jnp.exp(-v))
        scaled = (r * (total * sg * (1.0 + v * (1.0 - sg)))).astype(BF)
        kappa = r * jnp.sum(scaled.astype(F32) * v, axis=-1, keepdims=True) * (1.0 / D)
        pgb[l, x, :, :LAT] = scaled
        pgb[l, x, :, LAT:] = split_lanes(kappa)
        base = broadcast(pgb, l)
        emit_next()
        wgrad(l, 1, g, l + 1, act, out_scale)
        yield
        collect(pgb, l, base)
        left = pgb[l, :, :, :LAT].reshape(128, LAT)
        kap = join_lanes(pgb[l, :, :, LAT:].reshape(128, EXT))

        if l < 2:
            input_grads(l)

        def body(i, carry):
            c = pl.multiple_of(i * NT, NT)
            right = W[l, 0, i].reshape(NT, 1024)
            old = g[l + 1, :, :, pl.ds(c, NT)].reshape(128, NT).astype(F32)
            base_h = h[l, :, :, pl.ds(c, NT)].reshape(128, NT).astype(F32)
            g[l, :, :, pl.ds(c, NT)] = (old + dot_nt(left, right) - base_h * kap).astype(BF).reshape(4, 32, NT)
            return carry
        lax.fori_loop(0, 4, body, 0, unroll=True)
        emit(g, l, l, ig_hbm)

    def input_grads(l):
        wgrad(l, 0, h, l, pgb, in_scale)
        gx_base[l] = sem("r")
        push(G.at[l, other], Gx.at[l], gx_base[l], partner)

    gx_base = {}

    def merge(l):
        got(Gx.at[l], gx_base[l])

        def body(i, carry):
            at = (l, core, i // 2, i % 2)
            G[at] = G[at] + Gx[l, i // 2, i % 2]
            return carry
        lax.fori_loop(0, 8, body, 0)

    def rs_ring(half, lands, q, to_plus, to_minus, parts, result):
        p1, m1, p2, m2 = lands
        base = sem("r", 6)
        qp, qm, qo = (q + 1) % 4, (q + 3) % 4, (q + 2) % 4
        push(half(qo, 0), p1, base + 0, to_plus)
        push(half(qo, 1), m1, base + 1, to_minus)
        push(half(qp, 1), p2(1), base + 2, to_plus)
        push(half(qm, 0), m2(0), base + 3, to_minus)
        yield
        got(p1, base + 0)
        parts(half(qp, 0), half(qp, 0), [p1])
        push(half(qp, 0), p2(0), base + 4, to_plus)
        got(m1, base + 1)
        parts(half(qm, 1), half(qm, 1), [m1])
        push(half(qm, 1), m2(1), base + 5, to_minus)
        yield
        got(m2(0), base + 3)
        got(p2(0), base + 4)
        parts(half(q, 0), result(0), [p2(0), m2(0)])
        got(p2(1), base + 2)
        got(m2(1), base + 5)
        parts(half(q, 1), result(1), [p2(1), m2(1)])

    def add_flat(shape):
        count = math.prod(shape)

        def run(own, out, terms):
            def body(i, carry):
                index, rest = [], i
                for n in reversed(shape):
                    index.insert(0, rest % n)
                    rest = rest // n
                index = tuple(index)
                value = own[index] if index else own[...]
                value = value.astype(F32)
                for t in terms:
                    value = value + (t[index] if index else t[...]).astype(F32)
                if index:
                    out[index] = value.astype(BF)
                else:
                    out[...] = value.astype(BF)
                return carry
            lax.fori_loop(0, count, body, 0)
        return run

    def reduce_round(l):
        def half_a1(c, n):
            return G.at[l, core, c, n, :, 0]

        def half_b1(c, n):
            return G.at[l, core, 2 * n:2 * n + 2, c % 2, c // 2, 1]

        a1 = (z1.at[l, 0, 0], z1.at[l, 0, 1], lambda n: z2.at[l, 0, 0, n], lambda n: z2.at[l, 0, 1, n])
        b1 = (z1.at[l, 1, 0], z1.at[l, 1, 1], lambda n: z2.at[l, 1, 0, n], lambda n: z2.at[l, 1, 1, n])
        yield from zipped([
            rs_ring(half_a1, a1, z, to_zp, to_zm, add_flat((2,)), lambda n: half_a1(z, n)),
            rs_ring(half_b1, b1, y, to_yp, to_ym, add_flat((2,)), lambda n: half_b1(y, n)),
        ])

        def half_a2(c, n):
            return G.at[l, core, z, c % 2, c // 2, 0, 16 * n:16 * n + 16]

        def half_b2(c, n):
            return G.at[l, core, c, yl, yh, 1, 16 * n:16 * n + 16]

        a2 = (za.at[l, 0, 0], za.at[l, 0, 1], lambda n: zb.at[l, 0, 0, n], lambda n: zb.at[l, 0, 1, n])
        b2 = (za.at[l, 1, 0], za.at[l, 1, 1], lambda n: zb.at[l, 1, 0, n], lambda n: zb.at[l, 1, 1, n])
        yield from zipped([
            rs_ring(half_a2, a2, y, to_yp, to_ym, add_flat(()), lambda n: half_a2(y, n)),
            rs_ring(half_b2, b2, z, to_zp, to_zm, add_flat(()), lambda n: half_b2(z, n)),
        ])
        mine = G.at[l, core, z, yl, yh]
        copy = pltpu.make_async_remote_copy(
            src_ref=mine, dst_ref=gw.at[core, yh], send_sem=s_send.at[sem("s")], recv_sem=s_recv.at[home + s],
            device_id=(l, f), device_id_type=MESH,
        )

        @pl.when(s != l)
        def _():
            copy.start()

        @pl.when(s == l)
        def _():
            gw[core, yh] = mine[...]
        sent_home.append((l, copy))

    home = sem("r", 4)
    sent_home = []

    def step(task, n=1):
        for _ in range(n):
            next(task, None)

    share()
    hbase = spread(hid, h, loads[2])
    gbase = spread(cot, g, loads[3])
    shared()
    ready = set()

    def gather():
        first, rest = gather_first(0, 0), gather_first(slice(1, 4), 1)
        step(first)
        step(rest)
        yield
        yield from first
        current = gather_second(0)
        step(current)
        yield from rest
        for l in range(4):
            step(current)
            following = gather_second(l + 1) if l < 3 else None
            if following is not None:
                step(following)
            yield
            drain(current)
            ready.add(l)
            yield
            current = following

    bulk = gather()

    def need(l):
        while l not in ready:
            step(bulk)
        settle(l)

    need(0)
    for d in (1, 3, 2):
        got(h.at[0, (x + 4 - d) % 4], hbase + d)
    for l in range(4):
        need(l)
        for n, _ in enumerate(forward(l)):
            step(bulk)
            if l == 3 and n == 1:
                for d in (1, 3, 2):
                    got(g.at[4, (x + 4 - d) % 4], gbase + d)
                begin(3)
    running = []

    def poll(tasks):
        for task in list(tasks):
            step(task)

    def launch(l):
        merge(l)
        running.append(reduce_round(l))
        step(running[-1])

    for l in (3, 2, 1, 0):
        for n, _ in enumerate(backward(l)):
            poll(running[:1])
            if n == 0 and l == 0:
                launch(1)
            if n == 1 and l in (2, 1):
                launch(l + 1)
        if POLL:
            poll(running[:POLL])
    poll(running)
    launch(0)
    while parts_due:
        emit_next(True)
    remaining = zipped(running)
    step(remaining)
    drain(remaining)
    for l, copy in sent_home:
        @pl.when(s != l)
        def _():
            copy.wait_send()
    for ds in range(1, 4):
        ss = (s + ds) % 4
        got(gw.at[ss % 2, ss // 2], home + ss)
    gw_ref[...] = gw[...].reshape(2, 128, LAT)
    for copy in sends:
        copy.wait_send()
    finish_emit()
    assert counters["s"] <= SENDS and counters["r"] <= RECVS and counters["l"] <= 8, counters


SENDS, RECVS = 384, 512
POLL = 0
EMIT_FROM = 0


def shards(hidden_in, out_grad, fast_in, fast_out, slow_in, slow_out):
    any_ = pl.BlockSpec(memory_space=pl.ANY)
    so, ig, gw = pl.pallas_call(
        relay,
        out_shape=(
            jax.ShapeDtypeStruct((4, 128, 1024), BF),
            jax.ShapeDtypeStruct((4, 128, 1024), BF),
            jax.ShapeDtypeStruct((2, 128, 1024), BF),
        ),
        in_specs=[any_] * 4,
        out_specs=(any_, any_, pl.BlockSpec(memory_space=pltpu.VMEM)),
        scratch_shapes=[
            pltpu.VMEM((128, 1024), F32),
            pltpu.VMEM((1024, 128), F32),
            pltpu.VMEM((32, 4096), BF),
            pltpu.VMEM((32, 4096), BF),
            pltpu.VMEM((2, 4, 32, 1024), BF),
            pltpu.VMEM((2, 2, 2, 32, 1024), BF),
            pltpu.VMEM((4, 2, 4, 2, 2, 2, 32, 1024), BF),
            pltpu.VMEM((4, 2, 4, 2, 2, 2, 32, 1024), BF),
            pltpu.VMEM((4, 4, 2, 2, 2, 32, 1024), BF),
            pltpu.VMEM((5, 4, 32, 1024), BF),
            pltpu.VMEM((5, 4, 32, 1024), BF),
            pltpu.VMEM((8, 4, 32, 1024 + EXT), BF),
            pltpu.VMEM((8, 4, 32, 1024 + EXT), BF),
            pltpu.VMEM((4, 4, 32, 1024), BF),
            pltpu.VMEM((4, 4, 32, 1024 + EXT), BF),
            pltpu.VMEM((4, 32, 1024), F32),
            pltpu.VMEM((4, 32, EXT), F32),
            pltpu.VMEM((4, 2, 2, 2, 32, 1024), BF),
            pltpu.VMEM((4, 2, 2, 2, 2, 32, 1024), BF),
            pltpu.VMEM((4, 2, 2, 16, 1024), BF),
            pltpu.VMEM((4, 2, 2, 2, 16, 1024), BF),
            pltpu.VMEM((2, 2, 2, 32, 1024), BF),
            pltpu.SemaphoreType.DMA((12,)),
            pltpu.SemaphoreType.DMA((SENDS,)),
            pltpu.SemaphoreType.DMA((RECVS,)),
        ],
        compiler_params=pltpu.CompilerParams(
            collective_id=0, has_side_effects=True, vmem_limit_bytes=67043328
        ),
        name="relay",
    )(hidden_in, out_grad, fast_in, fast_out)

    return pl.pallas_call(
        finish,
        out_shape=(
            jax.ShapeDtypeStruct((1, 128, 4096), BF),
            jax.ShapeDtypeStruct((1, 128, 4096), BF),
            jax.ShapeDtypeStruct((1, 128, 1024), F32),
            jax.ShapeDtypeStruct((1, 1024, 128), F32),
        ),
        in_specs=[any_] * 7,
        out_specs=(any_,) * 4,
        scratch_shapes=[
            pltpu.VMEM((2, 4, 128, 1024), BF),
            pltpu.VMEM((2, 128, 1024), BF),
            pltpu.VMEM((2, 128, 1024), F32),
            pltpu.VMEM((2, 1024, 128), F32),
            pltpu.VMEM((128, 1024), F32),
            pltpu.VMEM((1024, 128), F32),
            pltpu.SemaphoreType.DMA((16,)),
            pltpu.SemaphoreType.DMA((40,)),
        ],
        name="finish",
    )(so, ig, gw, fast_in, fast_out, slow_in, slow_out)


def finish(so, ig, gw, fi, fo, si, so_slow, o0, o1, o2, o3, acts, grads, wi, wo, ri, ro, insem, outsem):
    loads = []

    def load(src, dst):
        c = pltpu.make_async_copy(src, dst, insem.at[len(loads)])
        c.start()
        loads.append(c)
        return c

    weights = [load(gw, grads), load(fo.at[0], wo.at[0]), load(so_slow.at[0], wo.at[1]),
               load(fi.at[0], wi.at[0]), load(si.at[0], wi.at[1])]
    pieces = [[load(t.at[x], acts.at[k, x]) for x in range(4)] for k, t in enumerate((so, ig))]
    stores = []

    def store(src, dst):
        c = pltpu.make_async_copy(src, dst, outsem.at[len(stores)])
        c.start()
        stores.append(c)

    for k, out in enumerate((o0, o1)):
        for x in range(4):
            pieces[k][x].wait()
            for zz in range(4):
                at = zz * 1024 + x * 256
                store(acts.at[k, x, :, zz * 256:(zz + 1) * 256], out.at[0, :, at:at + 256])

    def synced(fast, slow, grad):
        return slow + MIX * ((fast - RATE * grad) - slow)

    for c in weights[:3]:
        c.wait()
    ro[...] = synced(wo[0], wo[1], grads[1].astype(F32).T)
    store(ro, o3.at[0])
    for c in weights[3:]:
        c.wait()
    ri[...] = synced(wi[0], wi[1], grads[0].astype(F32))
    store(ri, o2.at[0])
    for c in stores:
        c.wait()


def solution(mesh):
    placed = (
        P("fsdp", None), P("fsdp", None),
        P("section", "fsdp", None), P("section", None, "fsdp"),
        P("section", "fsdp", None), P("section", None, "fsdp"),
    )
    return jax.shard_map(
        shards, mesh=mesh, in_specs=placed,
        out_specs=(
            P("section", "fsdp", None), P("section", "fsdp", None),
            P("section", "fsdp", None), P("section", None, "fsdp"),
        ),
        check_vma=False,
    )
```

```python
import functools
import math

import jax
import jax.numpy as jnp
from jax import lax
from jax.experimental import pallas as pl
from jax.experimental.pallas import tpu as pltpu
from jax.sharding import PartitionSpec as P

EPS = 1e-05
RATE = 0.5
MIX = 0.5
MESH = pl.DeviceIdType.MESH
BF = jnp.bfloat16
F32 = jnp.float32
EXT = 128


def split_lanes(column):
    high = column.astype(BF)
    low = (column - high.astype(F32)).astype(BF)
    lane = lax.broadcasted_iota(jnp.int32, (column.shape[0], EXT), 1)
    return jnp.where(lane < EXT // 2, high.astype(F32), low.astype(F32)).astype(BF)


def join_lanes(lanes):
    return jnp.sum(lanes.astype(F32), axis=-1, keepdims=True) * (2.0 / EXT)


def relay(
    hid_hbm, cot_hbm, fin_hbm, fout_hbm,
    so_hbm, ig_hbm, gw_ref,
    fin, fout, hid, cot, stage0, own, W, G, Gx, h, g, stgs, lands, stg, land, act, pg0, pg1, pre, rinv,
    z1, z2, za, zb, gw,
    in_sem, s_send, s_recv,
):
    D, LAT = 4096, 1024
    in_scale, out_scale = 1.0 / math.sqrt(D), 1.0 / math.sqrt(LAT)
    s = lax.axis_index("section")
    f = lax.axis_index("fsdp")
    core, yh = s % 2, s // 2
    z, x, yl = f // 8, (f // 2) % 4, f % 2
    y = yh * 2 + yl
    other = 1 - core

    def dev(yy, zz, xx, cc):
        return ((yy // 2) * 2 + cc, zz * 8 + xx * 2 + yy % 2)

    counters = {"s": 0, "r": 0}
    sends = []

    def sem(kind, n=1):
        at = counters[kind]
        counters[kind] += n
        return at

    def push(src, dst, recv_index, to):
        copy = pltpu.make_async_remote_copy(
            src_ref=src, dst_ref=dst, send_sem=s_send.at[sem("s")], recv_sem=s_recv.at[recv_index],
            device_id=to, device_id_type=MESH,
        )
        copy.start()
        sends.append(copy)

    def got(dst, recv_index):
        pltpu.make_async_remote_copy(
            src_ref=dst, dst_ref=dst, send_sem=s_send.at[0], recv_sem=s_recv.at[recv_index],
            device_id=(s, f), device_id_type=MESH,
        ).wait_recv()

    rows = pl.ds(pl.multiple_of(s * 32, 32), 32)
    loads = [
        pltpu.make_async_copy(fin_hbm.at[0], fin, in_sem.at[0]),
        pltpu.make_async_copy(fout_hbm.at[0], fout, in_sem.at[1]),
        pltpu.make_async_copy(hid_hbm.at[rows], hid, in_sem.at[2]),
        pltpu.make_async_copy(cot_hbm.at[rows], cot, in_sem.at[3]),
    ]
    for c in loads:
        c.start()

    yp, ym, zp, zm = (y + 1) % 4, (y + 3) % 4, (z + 1) % 4, (z + 3) % 4
    to_yp, to_ym = dev(yp, z, x, core), dev(ym, z, x, core)
    to_zp, to_zm = dev(y, zp, x, core), dev(y, zm, x, core)
    partner = dev(y, z, x, other)
    barrier = pltpu.get_barrier_semaphore()
    greeted = [to_yp, to_ym, to_zp, to_zm]
    for ds in range(4):
        for dx in range(4):
            if ds or dx:
                greeted.append(((s + ds) % 4, z * 8 + ((x + dx) % 4) * 2 + yl))
    for to in greeted:
        pl.semaphore_signal(barrier, inc=1, device_id=to, device_id_type=MESH)
    pl.semaphore_wait(barrier, len(greeted))

    def xdev(d):
        return (s, z * 8 + ((x + d) % 4) * 2 + yl)

    def quarters(rows):
        return rows.astype(BF).reshape(2, 2, 32, LAT)

    mates = sem("r", 8)

    def share():
        for c, value in ((0, lambda: fin[...] * in_scale), (1, lambda: (fout[...] * out_scale).T)):
            loads[c].wait()
            own[c] = quarters(value())
            push(own.at[c, 1 - yh], W.at[s, c, z, yl, 1 - yh], mates + core, ((1 - yh) * 2 + c, f))
        push(own.at[:, yh], W.at[s, :, z, yl, yh], mates + 2, partner)
        W[s, 0, z, yl, yh] = own[0, yh]
        W[s, 1, z, yl, yh] = own[1, yh]

    def shared():
        far = pl.ds(2 * (1 - yh), 2)
        for c in range(2):
            got(W.at[2 * (1 - yh) + c, core, z, yl, yh], mates + c)
        push(W.at[far, core, z, yl, yh], W.at[far, core, z, yl, yh], mates + 3, partner)
        got(W.at[yh * 2 + other, :, z, yl, yh], mates + 2)
        pending.append((0, lambda: got(W.at[far, other, z, yl, yh], mates + 3)))

    def spread(source, target, load):
        load.wait()
        base = sem("r", 4)
        slot = 0 if target is h else 1
        for xx in range(4):
            for zz in range(4):
                stage0[slot, xx, :, zz * 256:(zz + 1) * 256] = source[:, zz * 1024 + xx * 256: zz * 1024 + (xx + 1) * 256]
        level = 0 if target is h else 4
        target[level, x] = stage0[slot, x]
        for d in (1, 3, 2):
            push(stage0.at[slot, (x + d) % 4], target.at[level, x], base + d, xdev(d))
        return base

    def ag_ring(item, half, q, to_plus, to_minus, level):
        base = sem("r", 10)
        qp, qm, qo = (q + 1) % 4, (q + 3) % 4, (q + 2) % 4
        push(half(q, 0), half(q, 0), base + 0, to_plus)
        push(half(q, 1), half(q, 1), base + 1, to_minus)
        push(half(q, 1), half(q, 1), base + 2, to_plus)
        push(half(q, 0), half(q, 0), base + 3, to_minus)
        yield
        got(half(qm, 0), base + 0)
        push(half(qm, 0), half(qm, 0), base + 4, to_plus)
        got(half(qp, 1), base + 1)
        push(half(qp, 1), half(qp, 1), base + 5, to_minus)
        got(half(qm, 1), base + 2)
        push(item(qm), item(qm), base + 6, partner)
        got(half(qp, 0), base + 3)
        push(item(qp), item(qp), base + 7, partner)
        yield
        got(half(qo, 0), base + 4)
        push(half(qo, 0), half(qo, 0), base + 8, partner)
        got(half(qo, 1), base + 5)
        push(half(qo, 1), half(qo, 1), base + 9, partner)
        pending.append((level, lambda: twin(item, half, q, base)))

    pending = []

    def twin(item, half, q, base):
        qp, qm, qo = (q + 1) % 4, (q + 3) % 4, (q + 2) % 4
        got(item(qm, other), base + 6)
        got(item(qp, other), base + 7)
        got(half(qo, 0, other), base + 8)
        got(half(qo, 1, other), base + 9)

    def settle(level):
        for entry in list(pending):
            if entry[0] <= level:
                entry[1]()
                pending.remove(entry)

    def gather_first(ls, level):
        def item_a(c, k=core):
            return W.at[ls, k, z, c % 2, c // 2, 0]

        def half_a(c, n, k=core):
            return W.at[ls, k, z, c % 2, c // 2, 0, 16 * n:16 * n + 16]

        def item_b(c, k=core):
            return W.at[ls, k, c, yl, yh, 1]

        def half_b(c, n, k=core):
            return W.at[ls, k, c, yl, yh, 1, 16 * n:16 * n + 16]

        return zipped([
            ag_ring(item_a, half_a, y, to_yp, to_ym, level), ag_ring(item_b, half_b, z, to_zp, to_zm, level)])

    def gather_second(l):
        def item_a(c, k=core):
            return W.at[l, k, c, :, :, 0]

        def half_a(c, n, k=core):
            return W.at[l, k, c, n, :, 0]

        def item_b(c, k=core):
            return W.at[l, k, :, c % 2, c // 2, 1]

        def half_b(c, n, k=core):
            return W.at[l, k, 2 * n:2 * n + 2, c % 2, c // 2, 1]

        return zipped([
            ag_ring(item_a, half_a, z, to_zp, to_zm, l), ag_ring(item_b, half_b, y, to_yp, to_ym, l)])

    def zipped(tasks):
        tasks = list(tasks)
        while tasks:
            tasks = [t for t in tasks if next(t, True) is not True]
            if tasks:
                yield

    def drain(task):
        for _ in task:
            pass

    def dot_nn(a, b):
        return lax.dot_general(a, b, (((1,), (0,)), ((), ())), preferred_element_type=F32)

    def dot_nt(a, b):
        return lax.dot_general(a, b, (((1,), (1,)), ((), ())), preferred_element_type=F32)

    def dot_tn(a, b):
        return lax.dot_general(a, b, (((0,), (0,)), ((), ())), preferred_element_type=F32)

    NT = 256

    HALF = LAT // 2

    def slots(step, n, sums):
        if sums and n == 0:
            return stgs.at[step], lands.at[step]
        at = 2 * step + n
        return stg.at[at], land.at[at]

    def project(source, level, l, k, step, sums):
        left = source[level].reshape(128, 1024)
        base = sem("r", 8)
        for n in range(2):
            out, landing = slots(step, n, sums)
            for c in range(0, HALF, NT):
                right = W[l, k, :, :, :, :, :, n * HALF + c:n * HALF + c + NT].reshape(1024, NT)
                out[:, :, c:c + NT] = dot_nn(left, right).astype(BF).reshape(4, 32, NT)
            for d in (2, 1, 3):
                push(out.at[(x + d) % 4], landing.at[x], base + 4 * n + d, xdev(d))
            landing[x] = out[x]
        return base

    def summed(step, n, base, sums):
        landing = slots(step, n, sums)[1]
        for d in (1, 3, 2):
            got(landing.at[(x + 4 - d) % 4], base + 4 * n + d)
        total = landing[0].astype(F32)
        for xx in range(1, 4):
            total = total + landing[xx].astype(F32)
        return total

    def broadcast(buf, n, base):
        for d in (2, 1, 3):
            push(buf.at[x], buf.at[x], base + 4 * n + d, xdev(d))

    def collect(bufs, base):
        for n in range(2):
            for d in (1, 3, 2):
                got(bufs[n].at[(x + 4 - d) % 4], base + 4 * n + d)

    def full(bufs):
        return jnp.concatenate([b[:, :, :HALF].reshape(128, HALF) for b in bufs], axis=-1)

    def acts(l):
        return act.at[l, 0], act.at[l, 1]

    def grads(l):
        return pg0.at[l], pg1.at[l]

    def emit(source, level, l, out_ref):
        base = sem("r", 16)
        emitted.append((l, base, out_ref))

        def part(ds):
            for d in ds:
                src = source.at[level, (x + d) % 4]
                dst = out_ref.at[x, rows]
                to = (l, z * 8 + ((x + d) % 4) * 2 + yl)
                copy = pltpu.make_async_remote_copy(
                    src_ref=src, dst_ref=dst, send_sem=s_send.at[sem("s")], recv_sem=s_recv.at[base + s * 4 + x],
                    device_id=to, device_id_type=MESH,
                )
                if d:
                    copy.start()
                    sends.append(copy)
                else:
                    local = pltpu.make_async_copy(src, dst, in_sem.at[4 + sem("l")])

                    @pl.when(s != l)
                    def _():
                        copy.start()

                    @pl.when(s == l)
                    def _():
                        local.start()
                    locals_.append((l, copy, local))
        parts_due.append(lambda: part((0, 2)))
        parts_due.append(lambda: part((1, 3)))

    parts_due = []

    def emit_next(last=False):
        counters["w"] += 1
        if parts_due and (last or counters["w"] > EMIT_FROM):
            parts_due.pop(0)()

    counters["l"] = counters["w"] = 0
    locals_, emitted = [], []

    def finish_emit():
        for l, copy, local in locals_:
            @pl.when(s != l)
            def _():
                copy.wait_send()

            @pl.when(s == l)
            def _():
                local.wait()
        for l, base, out_ref in emitted:
            @pl.when(s == l)
            def _():
                for ds in range(4):
                    for dx in range(4):
                        if ds or dx:
                            ss, xx = (s + ds) % 4, (x + dx) % 4
                            got(out_ref.at[xx, pl.ds(pl.multiple_of(ss * 32, 32), 32)], base + ss * 4 + xx)

    def forward(l):
        wide = h[l].reshape(128, 1024).astype(F32)
        ss = jnp.sum(wide * wide, axis=-1, keepdims=True)
        stgs[l, :, :, HALF:] = split_lanes(ss).reshape(4, 32, EXT)
        base = project(h, l, l, 0, l, True)
        emit_next()
        yield
        away = sem("r", 8)
        r = None
        for n in range(2):
            total = summed(l, n, base, True)
            if n == 0:
                r = lax.rsqrt(join_lanes(total[:, HALF:]) * (1.0 / D) + EPS)
                total = total[:, :HALF]
            v = total * r
            act[l, n, x] = (v / (1.0 + jnp.exp(-v))).astype(BF)
            broadcast(act.at[l, n], n, away)
            pre[l, :, n * HALF:(n + 1) * HALF] = v
        rinv[l] = jnp.broadcast_to(r, (32, EXT))
        emit_next()
        yield
        collect(acts(l), away)
        left = full(acts(l))

        def body(i, carry):
            c = pl.multiple_of(i * NT, NT)
            right = W[l, 1, i].reshape(NT, 1024)
            old = h[l, :, :, pl.ds(c, NT)].reshape(128, NT).astype(F32)
            h[l + 1, :, :, pl.ds(c, NT)] = (old + dot_nt(left, right)).astype(BF).reshape(4, 32, NT)
            return carry
        lax.fori_loop(0, 4, body, 0, unroll=True)
        emit(h, l + 1, l, so_hbm)

    def wgrad(l, kind, left_ref, left_level, right_ref, scale):
        right = full(right_ref(l))

        def body(i, carry):
            c = pl.multiple_of(i * 128, 128)
            left = left_ref[left_level, :, :, pl.ds(c, 128)].reshape(128, 128)
            value = (dot_tn(left, right) * scale).astype(BF)
            G[l, kind, i // 2, i % 2] = value.reshape(2, 2, 32, LAT)
            return carry
        lax.fori_loop(0, 8, body, 0, unroll=4)

    begun = {}

    def begin(l):
        begun[l] = project(g, l + 1, l, 1, 7 - l, False)

    def backward(l):
        step = 7 - l
        if l not in begun:
            begin(l)
        base = begun[l]
        emit_next()
        if 1 < l + 1 < 4 and l > 0:
            input_grads(l + 1)
        yield
        away = sem("r", 8)
        r = rinv[l][:, :1]
        dots = None
        for n in range(2):
            total = summed(step, n, base, False)
            v = pre[l, :, n * HALF:(n + 1) * HALF]
            sg = 1.0 / (1.0 + jnp.exp(-v))
            scaled = (r * (total * sg * (1.0 + v * (1.0 - sg)))).astype(BF)
            term = jnp.sum(scaled.astype(F32) * v, axis=-1, keepdims=True)
            dots = term if n == 0 else dots + term
            part = grads(l)[n]
            part[x, :, :HALF] = scaled
            if n:
                part[x, :, HALF:] = split_lanes(r * dots * (1.0 / D))
            broadcast(part, n, away)
        emit_next()
        wgrad(l, 1, g, l + 1, acts, out_scale)
        yield
        collect(grads(l), away)
        if l < 2:
            input_grads(l)
        left = full(grads(l))
        kap = join_lanes(pg1[l, :, :, HALF:].reshape(128, EXT))

        def body(i, carry):
            c = pl.multiple_of(i * NT, NT)
            right = W[l, 0, i].reshape(NT, 1024)
            old = g[l + 1, :, :, pl.ds(c, NT)].reshape(128, NT).astype(F32)
            base_h = h[l, :, :, pl.ds(c, NT)].reshape(128, NT).astype(F32)
            g[l, :, :, pl.ds(c, NT)] = (old + dot_nt(left, right) - base_h * kap).astype(BF).reshape(4, 32, NT)
            return carry
        lax.fori_loop(0, 4, body, 0, unroll=True)
        emit(g, l, l, ig_hbm)

    def input_grads(l):
        wgrad(l, 0, h, l, grads, in_scale)
        gx_base[l] = sem("r")
        push(G.at[l, other], Gx.at[l], gx_base[l], partner)

    gx_base = {}

    def merge(l):
        got(Gx.at[l], gx_base[l])

        def body(i, carry):
            at = (l, core, i // 2, i % 2)
            G[at] = G[at] + Gx[l, i // 2, i % 2]
            return carry
        lax.fori_loop(0, 8, body, 0)

    def rs_ring(half, lands, q, to_plus, to_minus, parts, result):
        p1, m1, p2, m2 = lands
        base = sem("r", 6)
        qp, qm, qo = (q + 1) % 4, (q + 3) % 4, (q + 2) % 4
        push(half(qo, 0), p1, base + 0, to_plus)
        push(half(qo, 1), m1, base + 1, to_minus)
        push(half(qp, 1), p2(1), base + 2, to_plus)
        push(half(qm, 0), m2(0), base + 3, to_minus)
        yield
        got(p1, base + 0)
        parts(half(qp, 0), half(qp, 0), [p1])
        push(half(qp, 0), p2(0), base + 4, to_plus)
        got(m1, base + 1)
        parts(half(qm, 1), half(qm, 1), [m1])
        push(half(qm, 1), m2(1), base + 5, to_minus)
        yield
        got(m2(0), base + 3)
        got(p2(0), base + 4)
        parts(half(q, 0), result(0), [p2(0), m2(0)])
        got(p2(1), base + 2)
        got(m2(1), base + 5)
        parts(half(q, 1), result(1), [p2(1), m2(1)])

    def add_flat(shape):
        count = math.prod(shape)

        def run(own, out, terms):
            def body(i, carry):
                index, rest = [], i
                for n in reversed(shape):
                    index.insert(0, rest % n)
                    rest = rest // n
                index = tuple(index)
                value = own[index] if index else own[...]
                value = value.astype(F32)
                for t in terms:
                    value = value + (t[index] if index else t[...]).astype(F32)
                if index:
                    out[index] = value.astype(BF)
                else:
                    out[...] = value.astype(BF)
                return carry
            lax.fori_loop(0, count, body, 0)
        return run

    def reduce_round(l):
        def half_a1(c, n):
            return G.at[l, core, c, n, :, 0]

        def half_b1(c, n):
            return G.at[l, core, 2 * n:2 * n + 2, c % 2, c // 2, 1]

        a1 = (z1.at[l, 0, 0], z1.at[l, 0, 1], lambda n: z2.at[l, 0, 0, n], lambda n: z2.at[l, 0, 1, n])
        b1 = (z1.at[l, 1, 0], z1.at[l, 1, 1], lambda n: z2.at[l, 1, 0, n], lambda n: z2.at[l, 1, 1, n])
        yield from zipped([
            rs_ring(half_a1, a1, z, to_zp, to_zm, add_flat((2,)), lambda n: half_a1(z, n)),
            rs_ring(half_b1, b1, y, to_yp, to_ym, add_flat((2,)), lambda n: half_b1(y, n)),
        ])

        def half_a2(c, n):
            return G.at[l, core, z, c % 2, c // 2, 0, 16 * n:16 * n + 16]

        def half_b2(c, n):
            return G.at[l, core, c, yl, yh, 1, 16 * n:16 * n + 16]

        a2 = (za.at[l, 0, 0], za.at[l, 0, 1], lambda n: zb.at[l, 0, 0, n], lambda n: zb.at[l, 0, 1, n])
        b2 = (za.at[l, 1, 0], za.at[l, 1, 1], lambda n: zb.at[l, 1, 0, n], lambda n: zb.at[l, 1, 1, n])
        yield from zipped([
            rs_ring(half_a2, a2, y, to_yp, to_ym, add_flat(()), lambda n: half_a2(y, n)),
            rs_ring(half_b2, b2, z, to_zp, to_zm, add_flat(()), lambda n: half_b2(z, n)),
        ])
        mine = G.at[l, core, z, yl, yh]
        copy = pltpu.make_async_remote_copy(
            src_ref=mine, dst_ref=gw.at[core, yh], send_sem=s_send.at[sem("s")], recv_sem=s_recv.at[home + s],
            device_id=(l, f), device_id_type=MESH,
        )

        @pl.when(s != l)
        def _():
            copy.start()

        @pl.when(s == l)
        def _():
            gw[core, yh] = mine[...]
        sent_home.append((l, copy))

    home = sem("r", 4)
    sent_home = []

    def step(task, n=1):
        for _ in range(n):
            next(task, None)

    share()
    hbase = spread(hid, h, loads[2])
    gbase = spread(cot, g, loads[3])
    shared()
    ready = set()

    def gather():
        first, rest = gather_first(0, 0), gather_first(slice(1, 4), 1)
        step(first)
        step(rest)
        yield
        yield from first
        current = gather_second(0)
        step(current)
        yield from rest
        for l in range(4):
            step(current)
            following = gather_second(l + 1) if l < 3 else None
            if following is not None:
                step(following)
            yield
            drain(current)
            ready.add(l)
            yield
            current = following

    bulk = gather()

    def need(l):
        while l not in ready:
            step(bulk)
        settle(l)

    need(0)
    for d in (1, 3, 2):
        got(h.at[0, (x + 4 - d) % 4], hbase + d)
    for l in range(4):
        need(l)
        for n, _ in enumerate(forward(l)):
            step(bulk)
            if l == 3 and n == 1:
                for d in (1, 3, 2):
                    got(g.at[4, (x + 4 - d) % 4], gbase + d)
                begin(3)
    running = []

    def poll(tasks):
        for task in list(tasks):
            step(task)

    def launch(l):
        merge(l)
        running.append(reduce_round(l))
        step(running[-1])

    for l in (3, 2, 1, 0):
        for n, _ in enumerate(backward(l)):
            poll(running[:1])
            if n == 0 and l == 0:
                launch(1)
            if n == 1 and l in (2, 1):
                launch(l + 1)
        if POLL:
            poll(running[:POLL])
    poll(running)
    launch(0)
    while parts_due:
        emit_next(True)
    remaining = zipped(running)
    step(remaining)
    drain(remaining)
    for l, copy in sent_home:
        @pl.when(s != l)
        def _():
            copy.wait_send()
    for ds in range(1, 4):
        ss = (s + ds) % 4
        got(gw.at[ss % 2, ss // 2], home + ss)
    gw_ref[...] = gw[...].reshape(2, 128, LAT)
    for copy in sends:
        copy.wait_send()
    finish_emit()
    assert counters["s"] <= SENDS and counters["r"] <= RECVS and counters["l"] <= 8, counters


SENDS, RECVS = 384, 512
POLL = 0
EMIT_FROM = 0


def shards(hidden_in, out_grad, fast_in, fast_out, slow_in, slow_out):
    any_ = pl.BlockSpec(memory_space=pl.ANY)
    so, ig, gw = pl.pallas_call(
        relay,
        out_shape=(
            jax.ShapeDtypeStruct((4, 128, 1024), BF),
            jax.ShapeDtypeStruct((4, 128, 1024), BF),
            jax.ShapeDtypeStruct((2, 128, 1024), BF),
        ),
        in_specs=[any_] * 4,
        out_specs=(any_, any_, pl.BlockSpec(memory_space=pltpu.VMEM)),
        scratch_shapes=[
            pltpu.VMEM((128, 1024), F32),
            pltpu.VMEM((1024, 128), F32),
            pltpu.VMEM((32, 4096), BF),
            pltpu.VMEM((32, 4096), BF),
            pltpu.VMEM((2, 4, 32, 1024), BF),
            pltpu.VMEM((2, 2, 2, 32, 1024), BF),
            pltpu.VMEM((4, 2, 4, 2, 2, 2, 32, 1024), BF),
            pltpu.VMEM((4, 2, 4, 2, 2, 2, 32, 1024), BF),
            pltpu.VMEM((4, 4, 2, 2, 2, 32, 1024), BF),
            pltpu.VMEM((5, 4, 32, 1024), BF),
            pltpu.VMEM((5, 4, 32, 1024), BF),
            pltpu.VMEM((4, 4, 32, 512 + EXT), BF),
            pltpu.VMEM((4, 4, 32, 512 + EXT), BF),
            pltpu.VMEM((16, 4, 32, 512), BF),
            pltpu.VMEM((16, 4, 32, 512), BF),
            pltpu.VMEM((4, 2, 4, 32, 512), BF),
            pltpu.VMEM((4, 4, 32, 512), BF),
            pltpu.VMEM((4, 4, 32, 512 + EXT), BF),
            pltpu.VMEM((4, 32, 1024), F32),
            pltpu.VMEM((4, 32, EXT), F32),
            pltpu.VMEM((4, 2, 2, 2, 32, 1024), BF),
            pltpu.VMEM((4, 2, 2, 2, 2, 32, 1024), BF),
            pltpu.VMEM((4, 2, 2, 16, 1024), BF),
            pltpu.VMEM((4, 2, 2, 2, 16, 1024), BF),
            pltpu.VMEM((2, 2, 2, 32, 1024), BF),
            pltpu.SemaphoreType.DMA((12,)),
            pltpu.SemaphoreType.DMA((SENDS,)),
            pltpu.SemaphoreType.DMA((RECVS,)),
        ],
        compiler_params=pltpu.CompilerParams(
            collective_id=0, has_side_effects=True, vmem_limit_bytes=67043328
        ),
        name="relay",
    )(hidden_in, out_grad, fast_in, fast_out)

    return pl.pallas_call(
        finish,
        out_shape=(
            jax.ShapeDtypeStruct((1, 128, 4096), BF),
            jax.ShapeDtypeStruct((1, 128, 4096), BF),
            jax.ShapeDtypeStruct((1, 128, 1024), F32),
            jax.ShapeDtypeStruct((1, 1024, 128), F32),
        ),
        in_specs=[any_] * 7,
        out_specs=(any_,) * 4,
        scratch_shapes=[
            pltpu.VMEM((2, 4, 128, 1024), BF),
            pltpu.VMEM((2, 128, 1024), BF),
            pltpu.VMEM((2, 128, 1024), F32),
            pltpu.VMEM((2, 1024, 128), F32),
            pltpu.VMEM((128, 1024), F32),
            pltpu.VMEM((1024, 128), F32),
            pltpu.SemaphoreType.DMA((16,)),
            pltpu.SemaphoreType.DMA((40,)),
        ],
        name="finish",
    )(so, ig, gw, fast_in, fast_out, slow_in, slow_out)


def finish(so, ig, gw, fi, fo, si, so_slow, o0, o1, o2, o3, acts, grads, wi, wo, ri, ro, insem, outsem):
    loads = []

    def load(src, dst):
        c = pltpu.make_async_copy(src, dst, insem.at[len(loads)])
        c.start()
        loads.append(c)
        return c

    weights = [load(gw, grads), load(fo.at[0], wo.at[0]), load(so_slow.at[0], wo.at[1]),
               load(fi.at[0], wi.at[0]), load(si.at[0], wi.at[1])]
    pieces = [[load(t.at[x], acts.at[k, x]) for x in range(4)] for k, t in enumerate((so, ig))]
    stores = []

    def store(src, dst):
        c = pltpu.make_async_copy(src, dst, outsem.at[len(stores)])
        c.start()
        stores.append(c)

    for k, out in enumerate((o0, o1)):
        for x in range(4):
            pieces[k][x].wait()
            for zz in range(4):
                at = zz * 1024 + x * 256
                store(acts.at[k, x, :, zz * 256:(zz + 1) * 256], out.at[0, :, at:at + 256])

    def synced(fast, slow, grad):
        return slow + MIX * ((fast - RATE * grad) - slow)

    for c in weights[:3]:
        c.wait()
    ro[...] = synced(wo[0], wo[1], grads[1].astype(F32).T)
    store(ro, o3.at[0])
    for c in weights[3:]:
        c.wait()
    ri[...] = synced(wi[0], wi[1], grads[0].astype(F32))
    store(ri, o2.at[0])
    for c in stores:
        c.wait()


def solution(mesh):
    placed = (
        P("fsdp", None), P("fsdp", None),
        P("section", "fsdp", None), P("section", None, "fsdp"),
        P("section", "fsdp", None), P("section", None, "fsdp"),
    )
    return jax.shard_map(
        shards, mesh=mesh, in_specs=placed,
        out_specs=(
            P("section", "fsdp", None), P("section", "fsdp", None),
            P("section", "fsdp", None), P("section", None, "fsdp"),
        ),
        check_vma=False,
    )
```
